32 devices in a mesh: seq: 8 (over y, x, core), head: 4 (over z).
Axes of the slice: x: 2, y: 2, z: 4, core: 2. Of those that a mesh axis runs over, the one named last changes fastest.
Arguments:
- tokens: bfloat16 [2, 4096, 2048], P(None, 'seq'), may hold values from -6 to 6
- cotangent: bfloat16 [2, 4096, 2048], P(None, 'seq'), may hold values from -6 to 6
- decay_rates: float32 [8], replicated, may hold values from 0 to 1, as said below
- retention_gain: float32 [2048], P('seq'), may hold values from 0.1 to 1.9
- channel_gain: float32 [2048], P('seq'), may hold values from 0.1 to 1.9
- query_weight: float32 [2048, 2048], P('seq', 'head'), may hold values from -0.125 to 0.125
- key_weight: float32 [2048, 2048], P('seq', 'head'), may hold values from -0.125 to 0.125
- value_weight: float32 [2048, 3456], P('seq', 'head'), may hold values from -0.125 to 0.125
- swish_weight: float32 [2048, 3456], P('seq', 'head'), may hold values from -0.125 to 0.125
- output_weight: float32 [3456, 2048], P('head', 'seq'), may hold values from -0.109375 to 0.109375
- gate_weight: float32 [2048, 3456], P('seq', 'head'), may hold values from -0.125 to 0.125
- up_weight: float32 [2048, 3456], P('seq', 'head'), may hold values from -0.125 to 0.125
- down_weight: float32 [3456, 2048], P('head', 'seq'), may hold values from -0.109375 to 0.109375
- query_moment: float32 [2048, 2048], P('seq', 'head'), may hold values from -24 to 24
- key_moment: float32 [2048, 2048], P('seq', 'head'), may hold values from -24 to 24
- value_moment: float32 [2048, 3456], P('seq', 'head'), may hold values from -24 to 24
- swish_moment: float32 [2048, 3456], P('seq', 'head'), may hold values from -24 to 24
- output_moment: float32 [3456, 2048], P('head', 'seq'), may hold values from -24 to 24
- gate_moment: float32 [2048, 3456], P('seq', 'head'), may hold values from -24 to 24
- up_moment: float32 [2048, 3456], P('seq', 'head'), may hold values from -24 to 24
- down_moment: float32 [3456, 2048], P('head', 'seq'), may hold values from -24 to 24
- retention_first: float32 [2048], P('seq'), may hold values from -24 to 24
- retention_second: float32 [2048], P('seq'), may hold values from 1 to 100
- channel_first: float32 [2048], P('seq'), may hold values from -24 to 24
- channel_second: float32 [2048], P('seq'), may hold values from 1 to 100
Outputs:
- block_out: bfloat16 [2, 4096, 2048], P(None, 'seq')
- input_gradient: bfloat16 [2, 4096, 2048], P(None, 'seq')
- retention_gain_gradient: float32 [2048], P('seq')
- channel_gain_gradient: float32 [2048], P('seq')
- query_gradient: float32 [2048, 2048], P('seq', 'head')
- key_gradient: float32 [2048, 2048], P('seq', 'head')
- value_gradient: float32 [2048, 3456], P('seq', 'head')
- swish_gradient: float32 [2048, 3456], P('seq', 'head')
- output_gradient: float32 [3456, 2048], P('head', 'seq')
- gate_gradient: float32 [2048, 3456], P('seq', 'head')
- up_gradient: float32 [2048, 3456], P('seq', 'head')
- down_gradient: float32 [3456, 2048], P('head', 'seq')
- retention_gain_updated: float32 [2048], P('seq')
- channel_gain_updated: float32 [2048], P('seq')
- query_updated: float32 [2048, 2048], P('seq', 'head')
- key_updated: float32 [2048, 2048], P('seq', 'head')
- value_updated: float32 [2048, 3456], P('seq', 'head')
- swish_updated: float32 [2048, 3456], P('seq', 'head')
- output_updated: float32 [3456, 2048], P('head', 'seq')
- gate_updated: float32 [2048, 3456], P('seq', 'head')
- up_updated: float32 [2048, 3456], P('seq', 'head')
- down_updated: float32 [3456, 2048], P('head', 'seq')
- query_moment_updated: float32 [2048, 2048], P('seq', 'head')
- key_moment_updated: float32 [2048, 2048], P('seq', 'head')
- value_moment_updated: float32 [2048, 3456], P('seq', 'head')
- swish_moment_updated: float32 [2048, 3456], P('seq', 'head')
- output_moment_updated: float32 [3456, 2048], P('head', 'seq')
- gate_moment_updated: float32 [2048, 3456], P('seq', 'head')
- up_moment_updated: float32 [2048, 3456], P('seq', 'head')
- down_moment_updated: float32 [3456, 2048], P('head', 'seq')
- retention_first_updated: float32 [2048], P('seq')
- retention_second_updated: float32 [2048], P('seq')
- channel_first_updated: float32 [2048], P('seq')
- channel_second_updated: float32 [2048], P('seq')
The draws below stay inside these ranges and needn't reach their ends.
Inputs may be any that keep to these rules, and one draw needn't show every extreme that they name: `decay_rates`: positive decay rates.
All inputs are finite; a program needn't handle non-finite values.
Results may differ from the reference program's by a relative error of at most 0.015.
The reference program's roundings to bfloat16 on the way count: a program that leaves them out, or rounds other values in their place, can miss the bound.
Values may be sent and summed in bfloat16 or wider, within the bound.
A program may use at most 256 MiB of HBM per device.

```python
import math
from functools import partial
import jax
import jax.numpy as jnp
from jax import lax

D = 2048
HEADS = 8
KEY = 256
VAL = 432
FF = 3456
BLK = 512
SEQS = 2
SEQ_LEN = 4096
QK = 2048
VW = 3456
N_SEQ = 8


def draw_decay_rates(key, part):
    first_key = jax.random.fold_in(key, 11)
    second_key = jax.random.fold_in(key, 12)
    third_key = jax.random.fold_in(key, 13)
    quick = jax.random.uniform(first_key, (HEADS,), jnp.float32, 1.0 / 50.0, 1.0 / 30.0)
    slow = jax.random.uniform(second_key, (HEADS,), jnp.float32, 0.2, 2.0) / SEQ_LEN
    picked = jax.random.randint(third_key, (HEADS,), 0, 2) == 1
    return jnp.where(picked, quick, slow)


def levels(own_key, dims, shards, least, top_value):
    loudness, own = 1.0, jax.random.fold_in(own_key, 6)
    for position, shards_of in shards:
        steps = jnp.exp(jax.random.uniform(jax.random.fold_in(own, position), (shards_of,), jnp.float32, least / len(shards), top_value / len(shards)))
        loudness = loudness * jnp.repeat(steps, dims[position] // shards_of).reshape([-1 if axis == position else 1 for axis in range(len(dims))])
    return loudness


def normal_values(key, shape, deviation, bound, cuts=(), kind=jnp.bfloat16):
    array = deviation * jax.random.normal(key, shape, jnp.float32)
    if cuts:
        array = array * levels(key, shape, cuts, -0.22, 0.18)
    return jnp.clip(array, -bound, bound).astype(kind)


def setup_inputs(seed: int = 0) -> dict:
    key_of = jax.random.split(jax.random.key(seed), 26)
    return {
        "tokens": normal_values(key_of[0], (SEQS, SEQ_LEN, D), 1.0, 6.0, ((1, 8),)),
        "cotangent": normal_values(key_of[1], (SEQS, SEQ_LEN, D), 1.0, 6.0, ((1, 8),)),
        "decay_rates": draw_decay_rates(jax.random.fold_in(key_of[25], 71), 0),
        "retention_gain": jnp.clip(1.0 + 0.18 * jax.random.normal(key_of[3], (D,), jnp.float32), 0.1, 1.9),
        "channel_gain": jnp.clip(1.0 + 0.18 * jax.random.normal(key_of[4], (D,), jnp.float32), 0.1, 1.9),
        "query_weight": normal_values(key_of[5], (D, QK), D ** -0.5, 0.125, ((0, 8), (1, 4)), jnp.float32),
        "key_weight": normal_values(key_of[6], (D, QK), D ** -0.5, 0.125, ((0, 8), (1, 4)), jnp.float32),
        "value_weight": normal_values(key_of[7], (D, VW), D ** -0.5, 0.125, ((0, 8), (1, 4)), jnp.float32),
        "swish_weight": normal_values(key_of[8], (D, VW), D ** -0.5, 0.125, ((0, 8), (1, 4)), jnp.float32),
        "output_weight": normal_values(key_of[9], (VW, D), VW ** -0.5, 0.109375, ((0, 4), (1, 8)), jnp.float32),
        "gate_weight": normal_values(key_of[10], (D, FF), D ** -0.5, 0.125, ((0, 8), (1, 4)), jnp.float32),
        "up_weight": normal_values(key_of[11], (D, FF), D ** -0.5, 0.125, ((0, 8), (1, 4)), jnp.float32),
        "down_weight": normal_values(key_of[12], (FF, D), FF ** -0.5, 0.109375, ((0, 4), (1, 8)), jnp.float32),
        "query_moment": normal_values(key_of[13], (D, QK), 4.0, 24.0, ((0, 8), (1, 4)), jnp.float32),
        "key_moment": normal_values(key_of[14], (D, QK), 4.0, 24.0, ((0, 8), (1, 4)), jnp.float32),
        "value_moment": normal_values(key_of[15], (D, VW), 4.0, 24.0, ((0, 8), (1, 4)), jnp.float32),
        "swish_moment": normal_values(key_of[16], (D, VW), 4.0, 24.0, ((0, 8), (1, 4)), jnp.float32),
        "output_moment": normal_values(key_of[17], (VW, D), 4.0, 24.0, ((0, 4), (1, 8)), jnp.float32),
        "gate_moment": normal_values(key_of[18], (D, FF), 4.0, 24.0, ((0, 8), (1, 4)), jnp.float32),
        "up_moment": normal_values(key_of[19], (D, FF), 4.0, 24.0, ((0, 8), (1, 4)), jnp.float32),
        "down_moment": normal_values(key_of[20], (FF, D), 4.0, 24.0, ((0, 4), (1, 8)), jnp.float32),
        "retention_first": normal_values(key_of[21], (D,), 4.0, 24.0, ((0, 8),), jnp.float32),
        "retention_second": jnp.clip(jnp.exp(math.log(100.0) - 4.6051702 * jax.random.uniform(key_of[22], (D,), jnp.float32) ** levels(key_of[22], (D,), ((0, 8),), -0.2, 0.2)), 1.0, 100.0),
        "channel_first": normal_values(key_of[23], (D,), 4.0, 24.0, ((0, 8),), jnp.float32),
        "channel_second": jnp.clip(jnp.exp(math.log(100.0) - 4.6051702 * jax.random.uniform(key_of[24], (D,), jnp.float32) ** levels(key_of[24], (D,), ((0, 8),), -0.2, 0.2)), 1.0, 100.0),
    }


highest_precision = lax.Precision.HIGHEST
log_base = math.log(10000.0)
coef_first = 3.4445
coef_second = -4.775
coef_third = 2.0315
muon_rate = 0.02
muon_scale = 0.2
adam_rate = 0.1

@jax.custom_vjp
def low_precision(v):
    return lax.optimization_barrier(v.astype(jnp.bfloat16)).astype(jnp.float32)

@jax.custom_vjp
def low_precision_backward(v):
    return v

def low_keep(v):
    return (low_precision(v), None)

def low_pass(kept, grad):
    return (grad,)

def back_keep(v):
    return (v, None)

def back_low(kept, grad):
    return (low_precision(grad),)
low_precision.defvjp(low_keep, low_pass)
low_precision_backward.defvjp(back_keep, back_low)

def rms_scale(values, scale_gain):
    return values * lax.rsqrt(lax.optimization_barrier(jnp.mean(values * values, axis=-1, keepdims=True)) + 1e-06) * scale_gain

def rotate(values, cosine_table, sine_table):
    column = lax.broadcasted_iota(jnp.int32, values.shape, values.ndim - 1)
    swapped = jnp.where(column % 2 == 0, -jnp.roll(values, -1, axis=-1), jnp.roll(values, 1, axis=-1))
    return values * cosine_table + swapped * sine_table

def gate_norm(retained_output, swish_in):
    scaled = retained_output * lax.rsqrt(lax.optimization_barrier(jnp.mean(retained_output * retained_output, axis=-1, keepdims=True)) + 1e-05)
    return jax.nn.silu(swish_in) * scaled.reshape(swish_in.shape)

def inner_activation(gate_in, up_in):
    return jax.nn.gelu(gate_in, approximate=False) * up_in

def matrix_product(left, right):
    return jnp.matmul(left, right, precision=highest_precision)

def rotation_tables(length):
    positions = jnp.arange(length, dtype=jnp.float32)
    pair_index = (jnp.arange(KEY) // 2).astype(jnp.float32)
    frequency = jnp.exp(-log_base * pair_index / (KEY // 2 - 1))
    angles = positions[:, None] * frequency[None, :]
    return (jnp.cos(angles)[:, None, :], jnp.sin(angles)[:, None, :])

def retention_sequence(query_rot, key_rot, value_heads, rates):
    steps_in = jnp.arange(BLK, dtype=jnp.float32)
    offsets = steps_in[:, None] - steps_in[None, :]
    decay_mask = jnp.where(offsets >= 0, jnp.exp(-rates[:, None, None] * jnp.maximum(offsets, 0.0)), 0.0)
    query_decay = jnp.exp(-rates[None, :] * (steps_in[:, None] + 1.0))
    key_decay = jnp.exp(-rates[None, :] * (BLK - 1.0 - steps_in[:, None]))
    block_decay = jnp.exp(-rates * BLK)

    def block_step(running_state, pieces):
        query_block, key_block, value_block_rows = pieces
        scores = jnp.einsum('thk,uhk->htu', query_block, key_block, precision=highest_precision)
        weights_low = low_precision(low_precision_backward(scores) * decay_mask)
        query_rows_decayed = low_precision(query_block * query_decay[:, :, None])
        key_rows_decayed = low_precision(key_block * key_decay[:, :, None])
        retained_output = jnp.einsum('htu,uhv->thv', weights_low, value_block_rows, precision=highest_precision)
        retained_output = retained_output + jnp.einsum('fel,ely->fey', query_rows_decayed, low_precision(running_state), precision=highest_precision)
        block_local_state = low_precision_backward(jnp.einsum('wzl,wza->zla', key_rows_decayed, value_block_rows, precision=highest_precision))
        return (block_decay[:, None, None] * running_state + block_local_state, retained_output)
    query_blocks = query_rot.reshape(N_SEQ, BLK, HEADS, KEY)
    key_blocks = key_rot.reshape(N_SEQ, BLK, HEADS, KEY)
    value_blocks = value_heads.reshape(N_SEQ, BLK, HEADS, VAL)
    initial = jnp.zeros((HEADS, KEY, VAL), jnp.float32)
    final_state, outputs = lax.scan(jax.checkpoint(block_step), initial, (query_blocks, key_blocks, value_blocks))
    return outputs.reshape(N_SEQ * BLK, HEADS, VAL)

def layer(rates, stream_all, retention_gain, channel_gain, query_weight, key_weight, value_weight, swish_weight, output_weight, gate_weight, up_weight, down_weight):
    retention_scale = low_precision(retention_gain)
    channel_scale = low_precision(channel_gain)
    query_low = low_precision(query_weight)
    key_low = low_precision(key_weight)
    value_low = low_precision(value_weight)
    swish_low = low_precision(swish_weight)
    output_low = low_precision(output_weight)
    gate_low = low_precision(gate_weight)
    up_low = low_precision(up_weight)
    down_low = low_precision(down_weight)
    cosine_table, sine_table = rotation_tables(SEQ_LEN)
    key_scale = KEY ** (-0.5)

    def one_sequence(stream):
        normed_one = low_precision(rms_scale(stream, retention_scale))
        queries = low_precision_backward(matrix_product(normed_one, query_low)).reshape(SEQ_LEN, HEADS, KEY)
        keys = low_precision_backward(matrix_product(normed_one, key_low)).reshape(SEQ_LEN, HEADS, KEY)
        values = low_precision(low_precision_backward(matrix_product(normed_one, value_low))).reshape(SEQ_LEN, HEADS, VAL)
        swish_in = low_precision_backward(matrix_product(normed_one, swish_low))
        query_rot = low_precision(rotate(queries, cosine_table, sine_table))
        key_rot = low_precision(rotate(keys, cosine_table, sine_table) * key_scale)
        retained_output = low_precision_backward(retention_sequence(query_rot, key_rot, values, rates))
        gated = low_precision(gate_norm(retained_output, swish_in))
        mixed = stream + low_precision_backward(matrix_product(gated, output_low))
        normed_two = low_precision(rms_scale(mixed, channel_scale))
        gate_pre = low_precision_backward(matrix_product(normed_two, gate_low))
        up_pre = low_precision_backward(matrix_product(normed_two, up_low))
        activated = low_precision(inner_activation(gate_pre, up_pre))
        return mixed + matrix_product(activated, down_low)
    return lax.map(jax.checkpoint(one_sequence), stream_all)

def orthogonal(block):
    current = low_precision(block)
    current = current / (jnp.sqrt(jnp.sum(current * current)) + 1e-07)
    for newton_step in range(5):
        rounded = low_precision(current)
        gram_matrix = jnp.matmul(rounded.T, rounded, precision=highest_precision)
        gram_low = low_precision(gram_matrix)
        polynomial = coef_second * gram_matrix + coef_third * jnp.matmul(gram_low, gram_low, precision=highest_precision)
        current = coef_first * current + jnp.matmul(rounded, low_precision(polynomial), precision=highest_precision)
    return low_precision(current)

def muon_matrix(weight, gradient, moment, block_width, by_rows):
    moment_updated = 0.95 * moment + gradient
    advance = gradient + 0.95 * moment_updated
    if by_rows:
        blocks = advance.reshape(HEADS, block_width, D).transpose(0, 2, 1)
    else:
        blocks = advance.reshape(D, HEADS, block_width).transpose(1, 0, 2)
    updates = lax.map(orthogonal, blocks)
    if by_rows:
        update_full = updates.transpose(0, 2, 1).reshape(HEADS * block_width, D)
    else:
        update_full = updates.transpose(1, 0, 2).reshape(D, HEADS * block_width)
    return (weight - muon_rate * muon_scale * math.sqrt(D) * update_full, moment_updated)

def adam_gain(scale_gain, gradient, first_moment, second_moment):
    first_updated = 0.9 * first_moment + 0.1 * gradient
    second_updated = 0.95 * second_moment + 0.05 * gradient * gradient
    return (scale_gain - adam_rate * first_updated / (jnp.sqrt(second_updated) + 1e-08), first_updated, second_updated)

def reference(tokens, cotangent, decay_rates, retention_gain, channel_gain, query_weight, key_weight, value_weight, swish_weight, output_weight, gate_weight, up_weight, down_weight, query_moment, key_moment, value_moment, swish_moment, output_moment, gate_moment, up_moment, down_moment, retention_first, retention_second, channel_first, channel_second):
    result, pullback = jax.vjp(partial(layer, decay_rates), tokens.astype(jnp.float32), retention_gain, channel_gain, query_weight, key_weight, value_weight, swish_weight, output_weight, gate_weight, up_weight, down_weight)
    gradients = pullback(cotangent.astype(jnp.float32))
    input_gradient = gradients[0].astype(jnp.bfloat16)
    retention_gain_gradient = gradients[1]
    channel_gain_gradient = gradients[2]
    query_gradient, key_gradient, value_gradient, swish_gradient = (gradients[3], gradients[4], gradients[5], gradients[6])
    output_gradient, gate_gradient, up_gradient, down_gradient = (gradients[7], gradients[8], gradients[9], gradients[10])
    retention_gain_updated, retention_first_updated, retention_second_updated = adam_gain(retention_gain, retention_gain_gradient, retention_first, retention_second)
    channel_gain_updated, channel_first_updated, channel_second_updated = adam_gain(channel_gain, channel_gain_gradient, channel_first, channel_second)
    query_updated, query_moment_updated = muon_matrix(query_weight, query_gradient, query_moment, KEY, False)
    key_updated, key_moment_updated = muon_matrix(key_weight, key_gradient, key_moment, KEY, False)
    value_updated, value_moment_updated = muon_matrix(value_weight, value_gradient, value_moment, VAL, False)
    swish_updated, swish_moment_updated = muon_matrix(swish_weight, swish_gradient, swish_moment, VAL, False)
    output_updated, output_moment_updated = muon_matrix(output_weight, output_gradient, output_moment, VAL, True)
    gate_updated, gate_moment_updated = muon_matrix(gate_weight, gate_gradient, gate_moment, FF // HEADS, False)
    up_updated, up_moment_updated = muon_matrix(up_weight, up_gradient, up_moment, FF // HEADS, False)
    down_updated, down_moment_updated = muon_matrix(down_weight, down_gradient, down_moment, FF // HEADS, True)
    return (result.astype(jnp.bfloat16), input_gradient, retention_gain_gradient, channel_gain_gradient, query_gradient, key_gradient, value_gradient, swish_gradient, output_gradient, gate_gradient, up_gradient, down_gradient, retention_gain_updated, channel_gain_updated, query_updated, key_updated, value_updated, swish_updated, output_updated, gate_updated, up_updated, down_updated, query_moment_updated, key_moment_updated, value_moment_updated, swish_moment_updated, output_moment_updated, gate_moment_updated, up_moment_updated, down_moment_updated, retention_first_updated, retention_second_updated, channel_first_updated, channel_second_updated)
```

```python
import functools
import math

import jax
import jax.numpy as jnp
from jax import lax
from jax.experimental import pallas as pl
from jax.experimental.pallas import tpu as pltpu
from jax.sharding import PartitionSpec as P

D = 2048
HEADS = 8
KEY = 256
VAL = 432
FF = 3456
FBLK = FF // HEADS
SEQS = 2

log_base = math.log(10000.0)
coef_first = 3.4445
coef_second = -4.775
coef_third = 2.0315
muon_rate = 0.02
muon_scale = 0.2
adam_rate = 0.1
bfloat = jnp.bfloat16
single = jnp.float32
MESH = pl.DeviceIdType.MESH
VMEM_ALL = 67043328


def mm(left, right, contract):
    return lax.dot_general(left, right, (contract, ((), ())), preferred_element_type=single)


def nn(left, right):
    return mm(left, right, ((1,), (0,)))


def nt(left, right):
    return mm(left, right, ((1,), (1,)))


def tn(left, right):
    return mm(left, right, ((0,), (0,)))


def core_groups():
    count = lax.axis_size("seq")
    return [list(range(start, count, 2)) for start in (0, 1)]


def sibling(array):
    count = lax.axis_size("seq")
    return lax.ppermute(array, "seq", [(i, i ^ 1) for i in range(count)])


def is_second():
    return lax.axis_index("seq") % 2 == 1


def chips_gathered(stacked):
    return lax.all_gather(stacked, "seq", axis=0, axis_index_groups=core_groups())


def gathered(stacked):
    own = chips_gathered(stacked)
    other = sibling(own)
    second = is_second()
    low = jnp.where(second, other, own)
    high = jnp.where(second, own, other)
    chips, kinds, rows, columns = own.shape
    return [
        jnp.stack([low[:, i], high[:, i]], axis=1).reshape(chips * 2 * rows, columns)
        for i in range(kinds)
    ]


def scattered(locals_):
    count = lax.axis_size("seq")
    second = is_second()
    own, other = [], []
    for array in locals_:
        parts = array.reshape(count // 2, 2, array.shape[0] // count, array.shape[1])
        own.append(jnp.where(second, parts[:, 1], parts[:, 0]))
        other.append(jnp.where(second, parts[:, 0], parts[:, 1]).astype(bfloat))
    received = sibling(jnp.stack(other, axis=1)).astype(single)
    pair = (jnp.stack(own, axis=1) + received).astype(bfloat)
    return lax.psum_scatter(
        pair, "seq", scatter_dimension=0, tiled=False, axis_index_groups=core_groups()
    ).astype(single)


def heads_total(partial_sum):
    return lax.psum(partial_sum.astype(bfloat), "head").astype(single)


def gain_total(local):
    count = lax.axis_size("seq")
    pieces = lax.all_to_all(local.reshape(count, -1), "seq", 0, 0, tiled=True)
    return lax.psum(jnp.sum(pieces, axis=0), "head")


def state_exchange(local, decay, reverse):
    count = lax.axis_size("seq")
    blocks, keys, vals = local.shape
    pieces = local.astype(bfloat).reshape(blocks, count, keys // count, vals)
    pieces = lax.all_to_all(pieces.transpose(1, 0, 2, 3), "seq", 0, 0, tiled=True)
    pieces = pieces.astype(single)
    running = jnp.zeros_like(pieces[0])
    states = [None] * count
    for step in range(count):
        position = count - 1 - step if reverse else step
        states[position] = running.astype(bfloat)
        running = decay * running + pieces[position]
    returned = lax.all_to_all(jnp.stack(states), "seq", 0, 0, tiled=True)
    return returned.transpose(1, 0, 2, 3).reshape(blocks, keys, vals)


def adam_gain(scale_gain, gradient, first_moment, second_moment):
    first_updated = 0.9 * first_moment + 0.1 * gradient
    second_updated = 0.95 * second_moment + 0.05 * gradient * gradient
    return (
        scale_gain - adam_rate * first_updated / (jnp.sqrt(second_updated) + 1e-08),
        first_updated,
        second_updated,
    )


def muon_group(gradients, moments, masters, widths, by_rows, shift):
    heads_here = HEADS // lax.axis_size("head")
    count = lax.axis_size("seq")
    row_count = gradients[0].shape[0]
    moments_updated, pieces, shown = [], [], []
    for gradient, moment, width, transposed in zip(gradients, moments, widths, by_rows):
        if transposed:
            shown.append(gradient.T)
        else:
            shown.append(gradient)
        new = 0.95 * moment + shown[-1]
        moments_updated.append(new)
        advance = shown[-1] + 0.95 * new
        if transposed:
            advance = advance.T
        blocks = advance.astype(bfloat).reshape(row_count, heads_here, width).transpose(1, 0, 2)
        pieces.append(jnp.pad(blocks, ((0, 0), (0, 0), (0, VAL - width))))
    outgoing = jnp.concatenate(pieces, axis=0)
    block_count = outgoing.shape[0]
    if count >= block_count:
        spacing = count // block_count
        place = shift % spacing
        outgoing = jnp.pad(
            outgoing[:, None], ((0, 0), (place, spacing - 1 - place), (0, 0), (0, 0))
        ).reshape(count, 1, row_count, VAL)
    else:
        owned = block_count // count
        outgoing = outgoing.reshape(owned, count, row_count, VAL).transpose(1, 0, 2, 3)
    received = lax.all_to_all(outgoing, "seq", split_axis=0, concat_axis=0, tiled=True)
    items = received.shape[1]
    results = [orthogonal(received[:, i].reshape(count * row_count, VAL)) for i in range(items)]
    spread = jnp.stack([r.reshape(count, row_count, VAL) for r in results], axis=1)
    returned = lax.all_to_all(spread, "seq", split_axis=0, concat_axis=0, tiled=True)
    if count >= block_count:
        updates = returned.reshape(block_count, spacing, row_count, VAL)[:, place]
    else:
        updates = returned.transpose(1, 0, 2, 3).reshape(block_count, row_count, VAL)
    updates = updates.astype(single) * (muon_rate * muon_scale * math.sqrt(D))
    updated = []
    for position, (master, width, transposed) in enumerate(zip(masters, widths, by_rows)):
        piece = updates[position * heads_here : (position + 1) * heads_here, :, :width]
        if transposed:
            change = piece.transpose(0, 2, 1).reshape(heads_here * width, row_count)
        else:
            change = piece.transpose(1, 0, 2).reshape(row_count, heads_here * width)
        updated.append(master - change)
    return shown, moments_updated, updated


def dot(left, right, contract):
    return lax.dot_general(left, right, (contract, ((), ())), preferred_element_type=single)

class Line:
    def __init__(self, upward, rows, half, part, land, sems):
        self.n = lax.axis_size("head")
        self.upward, self.rows, self.half = upward, rows, half
        self.part, self.land = part, land
        self.red_send, self.red_recv, self.cast_send, self.cast_recv = sems
        self.z = lax.axis_index("head")
        self.count = half // rows
    def near(self, flow):
        toward_top = (flow + self.upward) % 2
        return jnp.where(toward_top == 1, self.z, self.n - 1 - self.z)
    def ahead(self, flow):
        toward_top = (flow + self.upward) % 2
        return self.z + 2 * toward_top - 1
    def at(self, flow, c):
        return pl.ds(pl.multiple_of(flow * self.half + c * self.rows, self.rows), self.rows)
    def move(self, flow, c):
        return pltpu.make_async_remote_copy(
            src_ref=self.part.at[self.at(flow, c)], dst_ref=self.land.at[self.at(flow, c)],
            send_sem=self.red_send.at[flow, c], recv_sem=self.red_recv.at[flow, c],
            device_id={"head": self.ahead(flow)}, device_id_type=MESH)
    def back(self, flow, c):
        return pltpu.make_async_remote_copy(
            src_ref=self.land.at[self.at(flow, c)], dst_ref=self.land.at[self.at(flow, c)],
            send_sem=self.cast_send.at[flow, c], recv_sem=self.cast_recv.at[flow, c],
            device_id={"head": 2 * self.z - self.ahead(flow)}, device_id_type=MESH)
    def reduce(self, flow, c):
        near = self.near(flow)
        at = self.at(flow, c)
        @pl.when(near > 0)
        def _():
            self.move(flow, c).wait_recv()
            summed = (self.land[at, :].astype(single) + self.part[at, :].astype(single)).astype(bfloat)
            @pl.when(near == self.n - 1)
            def _():
                self.land[at, :] = summed
            @pl.when(near < self.n - 1)
            def _():
                self.part[at, :] = summed
        @pl.when(near < self.n - 1)
        def _(): self.move(flow, c).start()
        @pl.when(near == self.n - 1)
        def _(): self.back(flow, c).start()
    def cast(self, flow, c):
        near = self.near(flow)
        @pl.when(near < self.n - 1)
        def _():
            self.back(flow, c).wait_recv()
            @pl.when(near > 0)
            def _(): self.back(flow, c).start()
    def finish(self):
        def each(index, carry):
            flow, c = index // self.count, index % self.count
            near = self.near(flow)
            @pl.when(near < self.n - 1)
            def _(): self.move(flow, c).wait_send()
            @pl.when(near > 0)
            def _(): self.back(flow, c).wait_send()
            return carry
        lax.fori_loop(0, 2 * self.count, each, 0)

def enter():
    barrier = pltpu.get_barrier_semaphore()
    z, n = lax.axis_index("head"), lax.axis_size("head")
    @pl.when(z > 0)
    def _(): pl.semaphore_signal(barrier, inc=1, device_id={"head": z - 1}, device_id_type=MESH)
    @pl.when(z < n - 1)
    def _(): pl.semaphore_signal(barrier, inc=1, device_id={"head": z + 1}, device_id_type=MESH)
    pl.semaphore_wait(barrier, jnp.where((z > 0) & (z < n - 1), 2, 1))

def middle_kernel(rows, y_hbm, x_hbm, g_hbm, own_hbm, other_hbm, gain_ref,
                  total_hbm, n2_hbm, m_hbm, da_hbm, db_hbm, pd_hbm, dh_hbm, dy_hbm, gsum_ref,
                  y, x, g, wo, wg, wu, wd, part1, land1, part3, land3,
                  n2s, ms, das, dbs, pds, dhs, dys, in_sems, weight_sems, out_sems, *sems):
    full, width = x.shape
    half = full // 2
    big = 2 * rows
    one = Line(0, rows, half, part1, land1, sems[:4])
    two = Line(1, rows, half, part3, land3, sems[4:])
    count = half // rows
    n = one.n
    loads = [pltpu.make_async_copy(a, b, in_sems.at[i])
             for i, (a, b) in enumerate(((y_hbm, y), (x_hbm, x), (g_hbm, g)))]
    core = lax.axis_index("seq") % 2
    chips, _, block, _ = own_hbm.shape
    def weight_loads(kind, to):
        loads = []
        for side, (source, parity) in enumerate(((own_hbm, core), (other_hbm, 1 - core))):
            for chip in range(chips):
                at = pl.ds(pl.multiple_of((2 * chip + parity) * block, block), block)
                loads.append(pltpu.make_async_copy(source.at[chip, kind], to.at[at], weight_sems.at[kind, side, chip]))
        return loads
    weights = [weight_loads(kind, to) for kind, to in enumerate((wo, wg, wu, wd))]
    for load in [loads[0]] + weights[0] + loads[1:] + weights[1] + weights[2] + weights[3]: load.start()
    gsum_ref[...] = jnp.zeros_like(gsum_ref)
    enter()
    for load in [loads[0]] + weights[0]: load.wait()
    def project(index, carry):
        k, flow = index // 2, index % 2
        at = pl.ds(pl.multiple_of(flow * half + k * big, big), big)
        part1[at, :] = dot(y[at, :], wo[...], ((1,), (1,))).astype(bfloat)
        @pl.when(one.near(flow) == 0)
        def _():
            one.reduce(flow, 2 * k)
            one.reduce(flow, 2 * k + 1)
        return carry
    lax.fori_loop(0, count, project, 0)
    for load in loads[1:] + weights[1] + weights[2] + weights[3]: load.wait()
    outs = ((n2s, n2_hbm), (ms, m_hbm), (das, da_hbm), (dbs, db_hbm), (pds, pd_hbm))
    def out_copy(i, flow, at):
        return pltpu.make_async_copy(outs[i][0].at[flow], outs[i][1].at[at], out_sems.at[i, flow])
    def dh_copy(flow, at):
        return pltpu.make_async_copy(dhs.at[flow], dh_hbm.at[at], out_sems.at[5, flow])
    def dy_copy(flow, at):
        return pltpu.make_async_copy(dys.at[flow], dy_hbm.at[at], out_sems.at[6, flow])

    def normed(at):
        mixed = x[at, :].astype(single) + land1[at, :].astype(single)
        rho = lax.rsqrt(jnp.mean(mixed * mixed, axis=-1, keepdims=True) + 1e-06)
        return rho, mixed * rho

    def inner(flow, k):
        at = pl.ds(pl.multiple_of(flow * half + k * big, big), big)
        @pl.when(k > 0)
        def _():
            for i in range(5): out_copy(i, flow, at).wait()
        rho, standard = normed(at)
        n2 = (standard * gain_ref[...]).astype(bfloat)
        n2s[flow] = n2
        a = dot(n2, wg[...], ((1,), (0,)))
        b = dot(n2, wu[...], ((1,), (0,)))
        dm = dot(g[at, :], wd[...], ((1,), (0,)))
        phi = 0.5 * (1.0 + lax.erf(a * math.sqrt(0.5)))
        gelu = a * phi
        slope = phi + a * jnp.exp(-0.5 * a * a) * (1.0 / math.sqrt(2.0 * math.pi))
        m = (gelu * b).astype(bfloat)
        da = (dm * b * slope).astype(bfloat)
        db = (dm * gelu).astype(bfloat)
        ms[flow] = m
        das[flow] = da
        dbs[flow] = db
        p3 = dot(da, wg[...], ((1,), (1,))) + dot(db, wu[...], ((1,), (1,)))
        part3[at, :] = p3.astype(bfloat)
        gsum_ref[...] += jnp.sum(p3 * standard, axis=0, keepdims=True)
        pds[flow] = dot(m, wd[...], ((1,), (1,))).astype(bfloat)
        for i in range(5): out_copy(i, flow, at).start()

    def last(flow, k):
        at = pl.ds(pl.multiple_of(flow * half + k * big, big), big)
        @pl.when(k > 0)
        def _():
            dh_copy(flow, at).wait()
            dy_copy(flow, at).wait()
        rho, standard = normed(at)
        scaled = land3[at, :].astype(single) * gain_ref[...]
        dh = g[at, :].astype(single) + rho * (
            scaled - standard * jnp.mean(scaled * standard, axis=-1, keepdims=True))
        low = dh.astype(bfloat)
        dhs[flow] = low
        dys[flow] = dot(low, wo[...], ((1,), (0,)))
        dh_copy(flow, at).start()
        dy_copy(flow, at).start()

    lag = 1
    slots = count + 4 * (n - 1) + lag + 1
    def slot(index, carry):
        s, flow = index // 2, index % 2
        near = one.near(flow)
        r = s - near
        @pl.when((near > 0) & (r >= 0) & (r < count))
        def _(): one.reduce(flow, r)
        arrival = 2 * (n - 1) - near
        k = s - arrival
        @pl.when((k >= 0) & (k < count))
        def _():
            one.cast(flow, k)
            @pl.when(k % 2 == 1)
            def _(): inner(flow, k // 2)
        near3 = n - 1 - near
        q = s - arrival - lag
        @pl.when((q >= 0) & (q < count) & (q % 2 == 1))
        def _():
            two.reduce(flow, q - 1)
            two.reduce(flow, q)
        e = s - (3 * (n - 1) - lag * 0) - (n - 1 - near3) - lag
        @pl.when((e >= 0) & (e < count) & (e % 2 == 1))
        def _():
            two.cast(flow, e - 1)
            two.cast(flow, e)
            last(flow, e // 2)
        return carry
    lax.fori_loop(0, 2 * slots, slot, 0)
    total_copy = pltpu.make_async_copy(land1, total_hbm, in_sems.at[0])
    total_copy.start()
    one.finish()
    two.finish()
    for flow in (0, 1):
        at = pl.ds(flow * half, big)
        for i in range(5): out_copy(i, flow, at).wait()
        dh_copy(flow, at).wait()
        dy_copy(flow, at).wait()
    total_copy.wait()

def middle(y, x, g, own, other, gain, cid, rows=64):
    full, width = x.shape
    hidden = y.shape[1]
    half = full // 2
    count = half // rows
    big = 2 * rows
    any_ = pl.BlockSpec(memory_space=pl.ANY)
    vm = pl.BlockSpec(memory_space=pltpu.VMEM)
    S = jax.ShapeDtypeStruct
    V = pltpu.VMEM
    wide, slim = (full, width), (full, hidden)
    return pl.pallas_call(
        functools.partial(middle_kernel, rows),
        out_shape=[S(wide, bfloat), S(wide, bfloat), S(slim, bfloat), S(slim, bfloat), S(slim, bfloat),
                   S(wide, bfloat), S(wide, bfloat), S(slim, single), S((1, width), single)],
        in_specs=[any_] * 5 + [vm],
        out_specs=[any_] * 8 + [vm],
        scratch_shapes=[V(slim, bfloat), V(wide, bfloat), V(wide, bfloat)] + [V((width, hidden), bfloat)] * 4
            + [V(wide, bfloat)] * 4
            + [V((2, big, width), bfloat), V((2, big, hidden), bfloat), V((2, big, hidden), bfloat),
               V((2, big, hidden), bfloat), V((2, big, width), bfloat), V((2, big, width), bfloat), V((2, big, hidden), single)]
            + [pltpu.SemaphoreType.DMA((3,)), pltpu.SemaphoreType.DMA((4, 2, own.shape[0])), pltpu.SemaphoreType.DMA((7, 2))]
            + [pltpu.SemaphoreType.DMA((2, count))] * 8,
        compiler_params=pltpu.CompilerParams(collective_id=cid, has_side_effects=True, vmem_limit_bytes=VMEM_ALL),
        cost_estimate=pl.CostEstimate(flops=260 * 10**9, bytes_accessed=60 * 10**6, transcendentals=0),
    )(y, x, g, own, other, gain)


def others():
    me = lax.axis_index("seq")
    core = me + 1 - 2 * (me % 2)
    x = 2 - 4 * ((me // 2) % 2)
    y = 4 - 8 * (me // 4)
    return core, (me + x, me + y, me + x + y)

def greet(devices):
    barrier = pltpu.get_barrier_semaphore()
    for device in devices:
        pl.semaphore_signal(barrier, inc=1, device_id={"seq": device}, device_id_type=MESH)
    pl.semaphore_wait(barrier, len(devices))

def scatter_kernel(shape, *refs):
    lefts = len(shape)
    matrices = [(g, i) for g, kinds in enumerate(shape) for i in range(kinds)]
    k = len(matrices)
    refs = list(refs)
    take = lambda count: [refs.pop(0) for _ in range(count)]
    left_hbm, right_hbm, outs = take(lefts), take(k), take(k)
    left, right = take(lefts), take(k)
    near_stage, near_land, far_stage, far_land = take(k), take(k), take(k), take(k)
    load_sem, near_send, near_recv, far_send, far_recv = refs
    loads = [pltpu.make_async_copy(a, b, load_sem.at[i])
             for i, (a, b) in enumerate(zip(left_hbm + right_hbm, left + right))]
    for load in loads: load.start()
    me = lax.axis_index("seq")
    core, chips = others()
    greet((core, *chips))
    rows = outs[0].shape[0]
    for load in loads: load.wait()

    def near_copy(i, r):
        return pltpu.make_async_remote_copy(
            src_ref=near_stage[i].at[r], dst_ref=near_land[i].at[r], send_sem=near_send.at[i, r],
            recv_sem=near_recv.at[i, r], device_id={"seq": core}, device_id_type=MESH)
    def far_copy(i, r, device):
        return pltpu.make_async_remote_copy(
            src_ref=far_stage[i].at[r - 1], dst_ref=far_land[i].at[r - 1], send_sem=far_send.at[i, r - 1],
            recv_sem=far_recv.at[i, r - 1], device_id={"seq": device}, device_id_type=MESH)
    def away(r):
        x = 2 - 4 * ((me // 2) % 2)
        y = 4 - 8 * (me // 4)
        return (r % 2) * x + (r // 2) * y
    def block(g, device):
        columns = pl.ds(pl.multiple_of(device * rows, rows), rows)
        return left[g][:, columns].T
    def tiles(device, use):
        index = 0
        for g, kinds in enumerate(shape):
            turned = block(g, device)
            for _ in range(kinds):
                use(index, dot(turned, right[index][...], ((1,), (0,))))
                index += 1
    def step(t, carry):
        @pl.when(t < 4)
        def _():
            r = 3 - t
            def use(i, tile):
                near_stage[i][r] = tile.astype(bfloat)
                near_copy(i, r).start()
            tiles(core + away(r), use)
        @pl.when(t > 0)
        def _():
            r = 4 - t
            def use(i, tile):
                near_copy(i, r).wait_recv()
                pair = tile + near_land[i][r].astype(single)
                @pl.when(r > 0)
                def _():
                    far_stage[i][r - 1] = pair.astype(bfloat)
                    far_copy(i, r, me + away(r)).start()
                @pl.when(r == 0)
                def _(): outs[i][...] = pair
            tiles(me + away(r), use)
        return carry
    lax.fori_loop(0, 5, step, 0)
    for i in range(k):
        for r in (1, 2, 3): far_copy(i, r, me + away(r)).wait_recv()
        outs[i][...] += (far_land[i][0].astype(single) + far_land[i][1].astype(single)) + far_land[i][2].astype(single)
    for i in range(k):
        for r in range(4): near_copy(i, r).wait_send()
        for r in (1, 2, 3): far_copy(i, r, me + away(r)).wait_send()

def grads_scattered(groups, cid):
    shape = tuple(len(rights) for _, rights in groups)
    lefts = [left for left, _ in groups]
    rights = [right for _, rights in groups for right in rights]
    rows = lefts[0].shape[1] // lax.axis_size("seq")
    V = pltpu.VMEM
    any_ = pl.BlockSpec(memory_space=pl.ANY)
    vm = pl.BlockSpec(memory_space=pltpu.VMEM)
    k = len(rights)
    tile = lambda count: [V((count, rows, right.shape[1]), bfloat) for right in rights]
    return pl.pallas_call(
        functools.partial(scatter_kernel, shape),
        out_shape=[jax.ShapeDtypeStruct((rows, right.shape[1]), single) for right in rights],
        in_specs=[any_] * (len(lefts) + k),
        out_specs=[vm] * k,
        scratch_shapes=[V(a.shape, bfloat) for a in lefts + rights] + tile(4) + tile(4) + tile(3) + tile(3)
            + [pltpu.SemaphoreType.DMA((len(lefts) + k,)), pltpu.SemaphoreType.DMA((k, 4)), pltpu.SemaphoreType.DMA((k, 4)),
               pltpu.SemaphoreType.DMA((k, 3)), pltpu.SemaphoreType.DMA((k, 3))],
        compiler_params=pltpu.CompilerParams(collective_id=cid, has_side_effects=True, vmem_limit_bytes=VMEM_ALL),
        cost_estimate=pl.CostEstimate(flops=80 * 10**9, bytes_accessed=30 * 10**6, transcendentals=0),
    )(*lefts, *rights)


def orthogonal_kernel(x_ref, out_ref, current):
    height = x_ref.shape[0]
    piece = 256
    def total(i, carry):
        value = x_ref[pl.ds(pl.multiple_of(i * piece, piece), piece), :].astype(single)
        return carry + jnp.sum(value * value, axis=0, keepdims=True)
    squares = lax.fori_loop(0, height // piece, total, jnp.zeros((1, x_ref.shape[1]), single))
    norm = jnp.sqrt(jnp.sum(squares, axis=1, keepdims=True)) + 1e-07
    def start(i, carry):
        at = pl.ds(pl.multiple_of(i * piece, piece), piece)
        value = x_ref[at, :].astype(single) / norm
        current[at, :] = value
        out_ref[at, :] = value.astype(bfloat)
        return carry
    lax.fori_loop(0, height // piece, start, 0)
    def newton(step, carry):
        def gram(i, q):
            rounded = out_ref[pl.ds(pl.multiple_of(i * 512, 512), 512), :]
            return q + dot(rounded, rounded, ((0,), (0,)))
        q = lax.fori_loop(0, height // 512, gram, jnp.zeros((x_ref.shape[1],) * 2, single))
        low = q.astype(bfloat)
        poly = (coef_second * q + coef_third * dot(low, low, ((1,), (0,)))).astype(bfloat)
        def apply(i, carry):
            at = pl.ds(pl.multiple_of(i * piece, piece), piece)
            value = coef_first * current[at, :] + dot(out_ref[at, :], poly, ((1,), (0,)))
            current[at, :] = value
            out_ref[at, :] = value.astype(bfloat)
            return carry
        return lax.fori_loop(0, height // piece, apply, carry)
    lax.fori_loop(0, 5, newton, 0)

def orthogonal(block):
    vm = pl.BlockSpec(memory_space=pltpu.VMEM)
    return pl.pallas_call(
        orthogonal_kernel, out_shape=jax.ShapeDtypeStruct(block.shape, bfloat), in_specs=[vm], out_specs=vm,
        scratch_shapes=[pltpu.VMEM(block.shape, single)],
        compiler_params=pltpu.CompilerParams(vmem_limit_bytes=48 << 20),
        cost_estimate=pl.CostEstimate(flops=17 * 10**9, bytes_accessed=4 * 10**6, transcendentals=0),
    )(block)


def rotated(values, cosine, sine):
    width = values.shape[1]
    even = lax.broadcasted_iota(jnp.int32, values.shape, 1) % 2 == 0
    swapped = jnp.where(even, -pltpu.roll(values, width - 1, 1), pltpu.roll(values, 1, 1))
    return values * cosine + swapped * sine

def front_kernel(x_hbm, gain_ref, cos_ref, sin_ref, q_hbm, k_hbm, v_hbm, s_hbm,
                 q_full, k_full, v_full, s_full, gains, n1, qh, kh, vh, sh,
                 x, rho, wq, wk, wv, ws, fq, fk, fv, fs, aq, ak, av, as_, load_sem, store_sem, send_sem, recv_sem):
    masters = (q_hbm, v_hbm, k_hbm, s_hbm)
    singles = (fq, fv, fk, fs)
    lands = (wq, wv, wk, ws, gains)
    fulls = (q_full, v_full, k_full, s_full)
    accs = (aq, av, ak, as_)
    loads = [pltpu.make_async_copy(a, b, load_sem.at[i]) for i, (a, b) in enumerate(zip(masters + (x_hbm,), singles + (x,)))]
    for load in loads: load.start()
    me = lax.axis_index("seq")
    core, (by_x, by_y, by_both) = others()
    step = {1: 1 - 2 * (me % 2), 2: 2 - 4 * ((me // 2) % 2), 4: 4 - 8 * (me // 4)}
    def place(rel):
        return me + sum(step[bit] for bit in (1, 2, 4) if rel & bit)
    greet((core, by_x, by_y))
    sent = []
    def send(rel, i, to):
        there = lands[i].at[place(rel)]
        copy = pltpu.make_async_remote_copy(
            src_ref=there, dst_ref=there, send_sem=send_sem.at[rel ^ to, i, to // 2], recv_sem=recv_sem.at[rel ^ to, i],
            device_id={"seq": place(to)}, device_id_type=MESH)
        copy.start()
        sent.append(copy)
    def arrive(rel, i):
        here = lands[i].at[place(rel)]
        pltpu.make_async_remote_copy(
            src_ref=here, dst_ref=here, send_sem=send_sem.at[rel, i, 0], recv_sem=recv_sem.at[rel, i],
            device_id={"seq": core}, device_id_type=MESH).wait_recv()
    gains[me] = gain_ref[...].astype(bfloat).astype(single)
    for to in (2, 4, 1): send(0, 4, to)
    for i in range(4):
        loads[i].wait()
        lands[i][me] = singles[i][...].astype(bfloat)
        for to in (2, 4, 1): send(0, i, to)
    loads[4].wait()
    tokens = x.shape[0]
    piece = 256
    def scale(t, carry):
        at = pl.ds(pl.multiple_of(t * piece, piece), piece)
        value = x[at, :].astype(single)
        rho[at, :] = lax.rsqrt(jnp.mean(value * value, axis=-1, keepdims=True) + 1e-06)
        return carry
    lax.fori_loop(0, tokens // piece, scale, 0)
    rows = gain_ref.shape[1]
    def product(rel, first):
        low = place(rel) - me % 2
        columns = pl.ds(pl.multiple_of(low * rows, 2 * rows), 2 * rows)
        scales = jnp.concatenate([gains[low][0:1, :], gains[low + 1][0:1, :]], axis=1)
        weights = [lands[i][pl.ds(low, 2)].reshape(2 * rows, lands[i].shape[2]) for i in range(4)]
        def part(t, carry):
            at = pl.ds(pl.multiple_of(t * piece, piece), piece)
            normed = (x[at, columns].astype(single) * rho[at, :] * scales).astype(bfloat)
            n1[at, columns] = normed
            for i in range(4):
                value = dot(normed, lands[i][pl.ds(low, 2)].reshape(2 * rows, lands[i].shape[2]), ((1,), (0,)))
                if first: accs[i][at, :] = value
                else: accs[i][at, :] += value
            return carry
        lax.fori_loop(0, tokens // piece, part, 0)
    for i in (4, 0, 1, 2, 3): arrive(1, i)
    product(0, True)
    def relay(rel, i):
        arrive(rel, i)
        send(rel, i, 1)
        if rel == 2 and i in (0, 1, 4): send(rel, i, 4)
        if rel == 4 and i in (2, 3): send(rel, i, 2)
    for i in (4, 0, 1, 2, 3):
        relay(2, i)
        relay(4, i)
    for i in (4, 0, 1, 2, 3): arrive(3, i)
    product(2, False)
    for i in (4, 0, 1, 2, 3): arrive(5, i)
    product(4, False)
    for i in (4, 0, 2, 1, 3):
        arrive(6, i)
        send(6, i, 1)
    for i in (4, 0, 2, 1, 3): arrive(7, i)
    stores = [pltpu.make_async_copy(a, b, store_sem.at[i]) for i, (a, b) in enumerate(zip(lands[:4], fulls))]
    for store in stores: store.start()
    product(6, False)
    heads = qh.shape[0] // 2
    block = tokens // 2
    def finish(s, carry):
        at = pl.ds(pl.multiple_of(s * block, block), block)
        for h in range(heads):
            keys = slice(h * KEY, (h + 1) * KEY)
            qh[s * heads + h] = rotated(aq[at, keys], cos_ref[...], sin_ref[...]).astype(bfloat)
            kh[s * heads + h] = (rotated(ak[at, keys], cos_ref[...], sin_ref[...]) * KEY ** -0.5).astype(bfloat)
            vh[s * heads + h] = av[at, :][:, h * VAL : (h + 1) * VAL].astype(bfloat)
            sh[s * heads + h] = as_[at, :][:, h * VAL : (h + 1) * VAL]
        return carry
    lax.fori_loop(0, 2, finish, 0)
    for copy in sent: copy.wait_send()
    for store in stores: store.wait()

def front(x, gains, cosine, sine, wq, wk, wv, ws, cid):
    tokens, width = x.shape
    count = lax.axis_size("seq")
    rows = width // count
    block = tokens // 2
    heads = wq.shape[1] // KEY
    any_ = pl.BlockSpec(memory_space=pl.ANY)
    vm = pl.BlockSpec(memory_space=pltpu.VMEM)
    S, V = jax.ShapeDtypeStruct, pltpu.VMEM
    gathered = [(count, rows, w.shape[1]) for w in (wq, wk, wv, ws)]
    return pl.pallas_call(
        front_kernel,
        out_shape=[S(g, bfloat) for g in gathered] + [S((count, 8, rows), single), S(x.shape, bfloat),
            S((2 * heads, block, KEY), bfloat), S((2 * heads, block, KEY), bfloat), S((2 * heads, block, VAL), bfloat), S((2 * heads, block, VAL), single)],
        in_specs=[any_, vm, vm, vm] + [any_] * 4,
        out_specs=[any_] * 4 + [vm] * 6,
        scratch_shapes=[V(x.shape, bfloat), V((tokens, 1), single)] + [V(g, bfloat) for g in gathered]
            + [V(w.shape, single) for w in (wq, wk, wv, ws)] + [V((tokens, w.shape[1]), single) for w in (wq, wk, wv, ws)]
            + [pltpu.SemaphoreType.DMA((5,)), pltpu.SemaphoreType.DMA((4,)), pltpu.SemaphoreType.DMA((8, 5, 3)), pltpu.SemaphoreType.DMA((8, 5))],
        compiler_params=pltpu.CompilerParams(collective_id=cid, has_side_effects=True, vmem_limit_bytes=VMEM_ALL),
        cost_estimate=pl.CostEstimate(flops=70 * 10**9, bytes_accessed=40 * 10**6, transcendentals=0),
    )(x, gains, cosine, sine, wq, wk, wv, ws)


def peers():
    me = lax.axis_index("seq")
    core, (by_x, by_y, by_both) = others()
    turn = core - me
    return core, by_x, by_y, by_x + turn, by_y + turn, by_both, by_both + turn

def decays(rate, length):
    t = lax.broadcasted_iota(jnp.int32, (length, 1), 0).astype(single)
    u = lax.broadcasted_iota(jnp.int32, (1, length), 1).astype(single)
    offsets = t - u
    mask = jnp.where(offsets >= 0, jnp.exp(-rate * jnp.maximum(offsets, 0.0)), 0.0)
    return mask, jnp.exp(-rate * (t + 1.0)), jnp.exp(-rate * (length - 1.0 - t)), jnp.exp(-rate * length)

class Exchange:
    def __init__(self, stage, land, stage_two, land_two, sems):
        self.stage, self.land, self.stage_two, self.land_two = stage, land, stage_two, land_two
        self.sends, self.recvs, self.sends_two, self.recvs_two = sems
        self.me = lax.axis_index("seq")
        self.peers = peers()
    def copy(self, two, i):
        stage, land = (self.stage_two, self.land_two) if two else (self.stage, self.land)
        sends, recvs = (self.sends_two, self.recvs_two) if two else (self.sends, self.recvs)
        return pltpu.make_async_remote_copy(
            src_ref=stage.at[self.peers[i]], dst_ref=land.at[self.me], send_sem=sends.at[i],
            recv_sem=recvs.at[i], device_id={"seq": self.peers[i]}, device_id_type=MESH)
    def arrived(self, two, i):
        land = self.land_two if two else self.land
        recvs = self.recvs_two if two else self.recvs
        sends = self.sends_two if two else self.sends
        here = land.at[self.peers[i]]
        pltpu.make_async_remote_copy(
            src_ref=here, dst_ref=here, send_sem=sends.at[i], recv_sem=recvs.at[i],
            device_id={"seq": self.peers[i]}, device_id_type=MESH).wait_recv()
    def start(self):
        for i in reversed(range(7)): self.copy(False, i).start()
        self.land[self.me] = self.stage[self.me]
    def turn(self, decay, reverse):
        for i in range(7): self.arrived(False, i)
        count = self.stage.shape[0]
        def step(index, running):
            position = count - 1 - index if reverse else index
            self.stage_two[position] = running.astype(bfloat)
            return decay * running + self.land[position].astype(single)
        lax.fori_loop(0, count, step, jnp.zeros(self.stage.shape[1:], single))
        for i in reversed(range(7)): self.copy(True, i).start()
        self.land_two[self.me] = self.stage_two[self.me]
    def end(self):
        for i in range(7): self.arrived(True, i)
    def state(self, b):
        count, _, part, width = self.land_two.shape
        return self.land_two[:, b].reshape(count * part, width)
    def finish(self):
        for i in range(7):
            self.copy(False, i).wait_send()
            self.copy(True, i).wait_send()

def retain_kernel(heads, q, k, v, s, rates, y, o, weights, state, stage, land, stage_two, land_two, *sems):
    blocks, length = q.shape[0], q.shape[1]
    count = stage.shape[0]
    exchange = Exchange(stage, land, stage_two, land_two, sems)
    greet(exchange.peers)
    rate = lambda h: rates[pl.ds(h, 1), 0:1]
    def local(b, carry):
        _, _, kd, _ = decays(rate(b % heads), length)
        low = (k[b].astype(single) * kd).astype(bfloat)
        piece = dot(low, v[b], ((0,), (0,))).astype(bfloat)
        stage[:, pl.ds(b, 1)] = piece.reshape(count, 1, piece.shape[0] // count, piece.shape[1])
        return carry
    lax.fori_loop(0, blocks, local, 0)
    exchange.start()
    def inside(b, carry):
        mask, _, _, _ = decays(rate(b % heads), length)
        low = (dot(q[b], k[b], ((1,), (1,))) * mask).astype(bfloat)
        weights[b] = low
        o[b] = dot(low, v[b], ((1,), (0,)))
        return carry
    lax.fori_loop(0, blocks, inside, 0)
    head = lax.broadcasted_iota(jnp.int32, (blocks, 1, 1), 0) % heads
    whole = jnp.zeros((blocks, 1, 1), single)
    for h in range(heads):
        whole = jnp.where(head == h, jnp.exp(-rate(h) * length).reshape(1, 1, 1), whole)
    exchange.turn(whole, False)
    exchange.end()
    def outer(sequence, carry):
        parts = []
        for h in range(heads):
            b = sequence * heads + h
            _, qd, _, _ = decays(rate(h), length)
            incoming = exchange.state(b)
            state[b] = incoming
            total = o[b] + dot((q[b].astype(single) * qd).astype(bfloat), incoming, ((1,), (0,)))
            o[b] = total
            rho = lax.rsqrt(jnp.mean(total * total, axis=-1, keepdims=True) + 1e-05)
            gate = s[b]
            parts.append((gate * jax.nn.sigmoid(gate) * total * rho).astype(bfloat))
        at = pl.ds(pl.multiple_of(sequence * length, length), length)
        y[at, :] = jnp.concatenate(parts, axis=1)
        return carry
    lax.fori_loop(0, blocks // heads, outer, 0)
    exchange.finish()

def exchange_scratch(count, blocks, keys, vals):
    return [pltpu.VMEM((count, blocks, keys // count, vals), bfloat)] * 4 + [pltpu.SemaphoreType.DMA((7,))] * 4

def retain(q, k, v, s, rates, cid):
    blocks, length, keys = q.shape
    vals = v.shape[2]
    heads = rates.shape[0]
    count = lax.axis_size("seq")
    vm = pl.BlockSpec(memory_space=pltpu.VMEM)
    S = jax.ShapeDtypeStruct
    return pl.pallas_call(
        functools.partial(retain_kernel, heads),
        out_shape=[S((blocks // heads * length, heads * vals), bfloat), S((blocks, length, vals), single),
                   S((blocks, length, length), bfloat), S((blocks, keys, vals), bfloat)],
        in_specs=[vm] * 5, out_specs=[vm] * 4,
        scratch_shapes=exchange_scratch(count, blocks, keys, vals),
        compiler_params=pltpu.CompilerParams(collective_id=cid, has_side_effects=True, vmem_limit_bytes=48 << 20),
        cost_estimate=pl.CostEstimate(flops=40 * 10**9, bytes_accessed=20 * 10**6, transcendentals=0),
    )(q, k, v, s, jnp.broadcast_to(rates[:, None], (heads, 128)))

def scattered_products(groups, cid):
    if lax.axis_size("seq") == 8:
        return grads_scattered(groups, cid)
    sums = []
    for left, rights in groups:
        for right in rights:
            sums.append(scattered([tn(left, right)])[0])
    return sums


def by_block(array, heads):
    rows, columns = array.shape
    parts = array.reshape(SEQS, rows // SEQS, heads, columns // heads).transpose(0, 2, 1, 3)
    return parts.reshape(SEQS * heads, rows // SEQS, columns // heads)


def by_row(array):
    blocks, length, columns = array.shape
    heads = blocks // SEQS
    parts = array.reshape(SEQS, heads, length, columns).transpose(0, 2, 1, 3)
    return parts.reshape(SEQS * length, heads * columns)


def rotate(values, cosine, sine):
    column = lax.broadcasted_iota(jnp.int32, values.shape, values.ndim - 1)
    swapped = jnp.where(
        column % 2 == 0, -jnp.roll(values, -1, axis=-1), jnp.roll(values, 1, axis=-1)
    )
    return values * cosine + swapped * sine


def projected(x, retention_gain, channel_gain, cosine, sine, weights):
    width = x.shape[1]
    heads = HEADS // lax.axis_size("head")
    gains = jnp.stack([retention_gain, channel_gain])
    if lax.axis_size("seq") == 8:
        gains = jnp.pad(gains, ((0, 6), (0, 0)))
        *fulls, gains, normed, q, k, v, s = front(x, gains, cosine, sine, *weights, 3)
        fulls = [full.reshape(width, full.shape[2]) for full in fulls]
        return fulls, (gains[:, 0].reshape(-1), gains[:, 1].reshape(-1)), normed, (q, k, v, s)
    gains = lax.all_gather(gains.astype(bfloat), "seq", axis=1, tiled=True).astype(single)
    fulls = gathered(jnp.stack([weights[0].astype(bfloat), weights[1].astype(bfloat)]))
    fulls += gathered(jnp.stack([weights[2].astype(bfloat), weights[3].astype(bfloat)]))
    stream = x.astype(single)
    rho = lax.rsqrt(jnp.mean(stream * stream, axis=-1, keepdims=True) + 1e-06)
    normed = (stream * rho * gains[0]).astype(bfloat)
    q, k, v, s = [by_block(nn(normed, full), heads) for full in fulls]
    q = rotate(q, cosine, sine).astype(bfloat)
    k = (rotate(k, cosine, sine) * KEY ** (-0.5)).astype(bfloat)
    return fulls, (gains[0], gains[1]), normed, (q, k, v.astype(bfloat), s)


def factors(rates, length):
    steps = jnp.arange(length, dtype=single)
    offsets = steps[:, None] - steps[None, :]
    every = jnp.tile(rates, SEQS)[:, None, None]
    mask = jnp.where(offsets >= 0, jnp.exp(-every * jnp.maximum(offsets, 0.0)), 0.0)
    steps = steps[None, :, None]
    return mask, jnp.exp(-every * (steps + 1.0)), jnp.exp(-every * (length - 1.0 - steps)), jnp.exp(-every * length)


def batched(spec, left, right):
    return jnp.einsum(spec, left, right, preferred_element_type=single)


def retained(q, k, v, s, rates):
    if lax.axis_size("seq") == 8:
        return retain(q, k, v, s, rates, 4)
    mask, qd, kd, whole = factors(rates, q.shape[1])
    local = batched("buk,buv->bkv", (k.astype(single) * kd).astype(bfloat), v)
    incoming = state_exchange(local, whole, False)
    weights = (batched("btk,buk->btu", q, k) * mask).astype(bfloat)
    o = batched("btu,buv->btv", weights, v)
    o = o + batched("btk,bkv->btv", (q.astype(single) * qd).astype(bfloat), incoming)
    rho = lax.rsqrt(jnp.mean(o * o, axis=-1, keepdims=True) + 1e-05)
    gated = (s * jax.nn.sigmoid(s) * o * rho).astype(bfloat)
    return by_row(gated), o, weights, incoming


def unretained(gated_grad, q, k, v, s, o, weights, incoming, rates, cosine, sine):
    heads = rates.shape[0]
    mask, qd, kd, whole = factors(rates, q.shape[1])
    grad = by_block(gated_grad, heads)
    rho = lax.rsqrt(jnp.mean(o * o, axis=-1, keepdims=True) + 1e-05)
    sigmoid = jax.nn.sigmoid(s)
    ds = (grad * (o * rho) * (sigmoid * (1.0 + s * (1.0 - sigmoid)))).astype(bfloat)
    inner = grad * (s * sigmoid)
    do = (
        rho * (inner - o * (rho * rho * jnp.mean(inner * o, axis=-1, keepdims=True)))
    ).astype(bfloat)
    local = batched("btk,btv->bkv", (q.astype(single) * qd).astype(bfloat), do)
    outgoing = state_exchange(local, whole, True)
    score = (batched("btv,buv->btu", do, v) * mask).astype(bfloat)
    dv = batched("btu,btv->buv", weights, do)
    dv = dv + batched("buk,bkv->buv", (k.astype(single) * kd).astype(bfloat), outgoing)
    dq = batched("btu,buk->btk", score, k) + batched("btv,bkv->btk", do, incoming) * qd
    dk = batched("btu,btk->buk", score, q) + batched("buv,bkv->buk", v, outgoing) * kd
    dq = rotate(dq, cosine, -sine).astype(bfloat)
    dk = (rotate(dk, cosine, -sine) * KEY ** (-0.5)).astype(bfloat)
    return by_row(dq), by_row(dk), by_row(dv.astype(bfloat)), by_row(ds)


def shards(
    tokens,
    cotangent,
    decay_rates,
    retention_gain,
    channel_gain,
    query_weight,
    key_weight,
    value_weight,
    swish_weight,
    output_weight,
    gate_weight,
    up_weight,
    down_weight,
    query_moment,
    key_moment,
    value_moment,
    swish_moment,
    output_moment,
    gate_moment,
    up_moment,
    down_moment,
    retention_first,
    retention_second,
    channel_first,
    channel_second,
):
    heads_here = HEADS // lax.axis_size("head")
    seq_count, block_length, width = tokens.shape
    rows = seq_count * block_length
    own_four = chips_gathered(
        jnp.stack(
            [
                output_weight.astype(bfloat).T,
                gate_weight.astype(bfloat),
                up_weight.astype(bfloat),
                down_weight.astype(bfloat).T,
            ]
        )
    )
    upstream_low = cotangent.reshape(rows, width)
    positions = (lax.axis_index("seq") * block_length + jnp.arange(block_length)).astype(single)
    pair_index = (jnp.arange(KEY) // 2).astype(single)
    frequency = jnp.exp(-log_base * pair_index / (KEY // 2 - 1))
    angles = positions[:, None] * frequency[None, :]
    cosine, sine = jnp.cos(angles), jnp.sin(angles)
    rates = lax.dynamic_slice(decay_rates, (lax.axis_index("head") * heads_here,), (heads_here,))
    (
        (query_full, key_full, value_full, swish_full),
        (retention_scale, channel_scale),
        normed_low,
        (query_blocks, key_blocks, value_blocks, swish_blocks),
    ) = projected(
        tokens.reshape(rows, width),
        retention_gain,
        channel_gain,
        cosine,
        sine,
        [query_weight, key_weight, value_weight, swish_weight],
    )
    own_four, query_blocks = lax.optimization_barrier((own_four, query_blocks))
    other_four = sibling(own_four)
    gated_low, retained_blocks, weights_low, incoming_low = retained(
        query_blocks, key_blocks, value_blocks, swish_blocks, rates
    )
    stream = tokens.reshape(rows, width).astype(single)
    rho_one = lax.rsqrt(jnp.mean(stream * stream, axis=-1, keepdims=True) + 1e-06)
    (
        mixed_total,
        normed_two_low,
        activated_low,
        gate_low_grad,
        up_low_grad,
        down_partial,
        mixed_low,
        gated_grad,
        channel_local,
    ) = middle(
        gated_low,
        tokens.reshape(rows, width),
        upstream_low,
        own_four,
        other_four,
        channel_scale[None, :],
        1,
    )
    channel_sum = gain_total(channel_local[0])
    down_total = heads_total(down_partial)
    block_out = (stream + mixed_total.astype(single) + down_total).astype(bfloat)
    down_local = tn(upstream_low, activated_low)
    gate_local = tn(normed_two_low, gate_low_grad)
    up_local = tn(normed_two_low, up_low_grad)
    output_local = tn(mixed_low, gated_low)
    early = scattered([output_local, gate_local, up_local, down_local])
    query_low_grad, key_low_grad, value_low_grad, swish_low_grad = unretained(
        gated_grad,
        query_blocks,
        key_blocks,
        value_blocks,
        swish_blocks,
        retained_blocks,
        weights_low,
        incoming_low,
        rates,
        cosine,
        sine,
    )
    normed_one_partial = (
        nt(query_low_grad, query_full)
        + nt(key_low_grad, key_full)
        + nt(value_low_grad, value_full)
        + nt(swish_low_grad, swish_full)
    )
    late = scattered_products(
        [(normed_low, [query_low_grad, key_low_grad, value_low_grad, swish_low_grad])], 2
    )
    standard_one = stream * rho_one
    retention_sum = gain_total(jnp.sum(normed_one_partial * standard_one, axis=0))
    normed_one_partial, down_total = lax.optimization_barrier((normed_one_partial, down_total))
    block_out = (stream + mixed_total.astype(single) + down_total).astype(bfloat)
    normed_one_grad = heads_total(normed_one_partial)
    scaled_one = normed_one_grad * retention_scale
    input_gradient = (
        mixed_low.astype(single)
        + rho_one
        * (scaled_one - standard_one * jnp.mean(scaled_one * standard_one, axis=-1, keepdims=True))
    ).astype(bfloat)

    retention_gain_updated, retention_first_updated, retention_second_updated = adam_gain(
        retention_gain, retention_sum, retention_first, retention_second
    )
    channel_gain_updated, channel_first_updated, channel_second_updated = adam_gain(
        channel_gain, channel_sum, channel_first, channel_second
    )
    early_grads, early_moments, early_updated = muon_group(
        [early[0], early[1], early[2], early[3]],
        [output_moment, gate_moment, up_moment, down_moment],
        [output_weight, gate_weight, up_weight, down_weight],
        [VAL, FBLK, FBLK, FBLK],
        [True, False, False, True],
        0,
    )
    late_grads, late_moments, late_updated = muon_group(
        late,
        [query_moment, key_moment, value_moment, swish_moment],
        [query_weight, key_weight, value_weight, swish_weight],
        [KEY, KEY, VAL, VAL],
        [False, False, False, False],
        1,
    )
    whole = (seq_count, block_length, width)
    return (
        block_out.reshape(whole),
        input_gradient.reshape(whole),
        retention_sum,
        channel_sum,
        *late_grads,
        *early_grads,
        retention_gain_updated,
        channel_gain_updated,
        *late_updated,
        *early_updated,
        *late_moments,
        *early_moments,
        retention_first_updated,
        retention_second_updated,
        channel_first_updated,
        channel_second_updated,
    )


def solution(mesh):
    placed = (
        P(None, "seq", None),
        P(None, "seq", None),
        P(),
        P("seq"),
        P("seq"),
        P("seq", "head"),
        P("seq", "head"),
        P("seq", "head"),
        P("seq", "head"),
        P("head", "seq"),
        P("seq", "head"),
        P("seq", "head"),
        P("head", "seq"),
        P("seq", "head"),
        P("seq", "head"),
        P("seq", "head"),
        P("seq", "head"),
        P("head", "seq"),
        P("seq", "head"),
        P("seq", "head"),
        P("head", "seq"),
        P("seq"),
        P("seq"),
        P("seq"),
        P("seq"),
    )
    return jax.shard_map(
        shards,
        mesh=mesh,
        in_specs=placed,
        out_specs=(
            P(None, "seq", None),
            P(None, "seq", None),
            P("seq"),
            P("seq"),
            P("seq", "head"),
            P("seq", "head"),
            P("seq", "head"),
            P("seq", "head"),
            P("head", "seq"),
            P("seq", "head"),
            P("seq", "head"),
            P("head", "seq"),
            P("seq"),
            P("seq"),
            P("seq", "head"),
            P("seq", "head"),
            P("seq", "head"),
            P("seq", "head"),
            P("head", "seq"),
            P("seq", "head"),
            P("seq", "head"),
            P("head", "seq"),
            P("seq", "head"),
            P("seq", "head"),
            P("seq", "head"),
            P("seq", "head"),
            P("head", "seq"),
            P("seq", "head"),
            P("seq", "head"),
            P("head", "seq"),
            P("seq"),
            P("seq"),
            P("seq"),
            P("seq"),
        ),
        check_vma=False,
    )
```

```python
import functools
import math

import jax
import jax.numpy as jnp
from jax import lax
from jax.experimental import pallas as pl
from jax.experimental.pallas import tpu as pltpu
from jax.sharding import PartitionSpec as P

D = 2048
HEADS = 8
KEY = 256
VAL = 432
FF = 3456
FBLK = FF // HEADS
SEQS = 2

log_base = math.log(10000.0)
coef_first = 3.4445
coef_second = -4.775
coef_third = 2.0315
muon_rate = 0.02
muon_scale = 0.2
adam_rate = 0.1
bfloat = jnp.bfloat16
single = jnp.float32
MESH = pl.DeviceIdType.MESH
VMEM_ALL = 67043328


def mm(left, right, contract):
    return lax.dot_general(left, right, (contract, ((), ())), preferred_element_type=single)


def nn(left, right):
    return mm(left, right, ((1,), (0,)))


def nt(left, right):
    return mm(left, right, ((1,), (1,)))


def tn(left, right):
    return mm(left, right, ((0,), (0,)))


def core_groups():
    count = lax.axis_size("seq")
    return [list(range(start, count, 2)) for start in (0, 1)]


def sibling(array):
    count = lax.axis_size("seq")
    return lax.ppermute(array, "seq", [(i, i ^ 1) for i in range(count)])


def is_second():
    return lax.axis_index("seq") % 2 == 1


def chips_gathered(stacked):
    return lax.all_gather(stacked, "seq", axis=0, axis_index_groups=core_groups())


def halves_gathered(stacked):
    full = lax.all_gather(stacked, "seq", axis=2, tiled=True)
    kinds, columns, _ = full.shape
    full = full.reshape(kinds, columns, -1, 256).transpose(2, 0, 1, 3)
    even, odd = full[0::2], full[1::2]
    return jnp.where(is_second(), odd, even), jnp.where(is_second(), even, odd)


def gain_exchanged(local):
    count = lax.axis_size("seq")
    pieces = local.reshape(count, -1, local.shape[1])
    return lax.all_to_all(pieces, "seq", 0, 0, tiled=True)


def gain_summed(pieces):
    heads = lax.axis_size("head")
    total = jnp.sum(pieces, axis=0)
    bit = 1
    while bit < heads:
        total = total + lax.ppermute(total, "head", [(i, i ^ bit) for i in range(heads)])
        bit *= 2
    return total


def state_exchange(local, decay, reverse):
    count = lax.axis_size("seq")
    blocks, keys, vals = local.shape
    pieces = local.astype(bfloat).reshape(blocks, count, keys // count, vals)
    pieces = lax.all_to_all(pieces.transpose(1, 0, 2, 3), "seq", 0, 0, tiled=True)
    pieces = pieces.astype(single)
    running = jnp.zeros_like(pieces[0])
    states = [None] * count
    for step in range(count):
        position = count - 1 - step if reverse else step
        states[position] = running.astype(bfloat)
        running = decay * running + pieces[position]
    returned = lax.all_to_all(jnp.stack(states), "seq", 0, 0, tiled=True)
    return returned.transpose(1, 0, 2, 3).reshape(blocks, keys, vals)


def adam_gain(scale_gain, gradient, first_moment, second_moment):
    first_updated = 0.9 * first_moment + 0.1 * gradient
    second_updated = 0.95 * second_moment + 0.05 * gradient * gradient
    return (
        scale_gain - adam_rate * first_updated / (jnp.sqrt(second_updated) + 1e-08),
        first_updated,
        second_updated,
    )


def dot(left, right, contract):
    return lax.dot_general(left, right, (contract, ((), ())), preferred_element_type=single)

class Line:
    def __init__(self, upward, rows, half, part, land, sems):
        self.n = lax.axis_size("head")
        self.upward, self.rows, self.half = upward, rows, half
        self.part, self.land = part, land
        self.red_send, self.red_recv, self.cast_send, self.cast_recv = sems
        self.z = lax.axis_index("head")
        self.count = half // rows
    def near(self, flow):
        toward_top = (flow + self.upward) % 2
        return jnp.where(toward_top == 1, self.z, self.n - 1 - self.z)
    def ahead(self, flow):
        toward_top = (flow + self.upward) % 2
        return self.z + 2 * toward_top - 1
    def at(self, flow, c):
        return pl.ds(pl.multiple_of(flow * self.half + c * self.rows, self.rows), self.rows)
    def move(self, flow, c):
        return pltpu.make_async_remote_copy(
            src_ref=self.part.at[self.at(flow, c)], dst_ref=self.land.at[self.at(flow, c)],
            send_sem=self.red_send.at[flow, c], recv_sem=self.red_recv.at[flow, c],
            device_id={"head": self.ahead(flow)}, device_id_type=MESH)
    def back(self, flow, c):
        return pltpu.make_async_remote_copy(
            src_ref=self.land.at[self.at(flow, c)], dst_ref=self.land.at[self.at(flow, c)],
            send_sem=self.cast_send.at[flow, c], recv_sem=self.cast_recv.at[flow, c],
            device_id={"head": 2 * self.z - self.ahead(flow)}, device_id_type=MESH)
    def reduce(self, flow, c):
        near = self.near(flow)
        at = self.at(flow, c)
        @pl.when(near > 0)
        def _():
            self.move(flow, c).wait_recv()
            summed = (self.land[at, :].astype(single) + self.part[at, :].astype(single)).astype(bfloat)
            @pl.when(near == self.n - 1)
            def _():
                self.land[at, :] = summed
            @pl.when(near < self.n - 1)
            def _():
                self.part[at, :] = summed
        @pl.when(near < self.n - 1)
        def _(): self.move(flow, c).start()
        @pl.when(near == self.n - 1)
        def _(): self.back(flow, c).start()
    def cast(self, flow, c):
        near = self.near(flow)
        @pl.when(near < self.n - 1)
        def _():
            self.back(flow, c).wait_recv()
            @pl.when(near > 0)
            def _(): self.back(flow, c).start()
    def finish(self):
        def each(index, carry):
            flow, c = index // self.count, index % self.count
            near = self.near(flow)
            @pl.when(near < self.n - 1)
            def _(): self.move(flow, c).wait_send()
            @pl.when(near > 0)
            def _(): self.back(flow, c).wait_send()
            return carry
        lax.fori_loop(0, 2 * self.count, each, 0)

def enter():
    barrier = pltpu.get_barrier_semaphore()
    z, n = lax.axis_index("head"), lax.axis_size("head")
    @pl.when(z > 0)
    def _(): pl.semaphore_signal(barrier, inc=1, device_id={"head": z - 1}, device_id_type=MESH)
    @pl.when(z < n - 1)
    def _(): pl.semaphore_signal(barrier, inc=1, device_id={"head": z + 1}, device_id_type=MESH)
    pl.semaphore_wait(barrier, jnp.where((z > 0) & (z < n - 1), 2, 1))

def middle_kernel(rows, y_hbm, x_hbm, g_hbm, own_hbm, other_hbm, gain_ref,
                  total_hbm, n2_hbm, m_hbm, da_hbm, db_hbm, pd_hbm, dh_hbm, dy_hbm, gsum_ref,
                  y, x, g, wo, wg, wu, wd, part1, land1, part3, land3,
                  n2s, ms, das, dbs, pds, dhs, dys, in_sems, weight_sems, out_sems, *sems):
    full, width = x.shape
    half = full // 2
    big = 2 * rows
    one = Line(0, rows, half, part1, land1, sems[:4])
    two = Line(1, rows, half, part3, land3, sems[4:])
    count = half // rows
    n = one.n
    loads = [pltpu.make_async_copy(a, b, in_sems.at[i])
             for i, (a, b) in enumerate(((y_hbm, y), (x_hbm, x), (g_hbm, g)))]
    core = lax.axis_index("seq") % 2
    chips, _, _, block = own_hbm.shape
    def weight_loads(kind, to):
        loads = []
        for side, (source, parity) in enumerate(((own_hbm, core), (other_hbm, 1 - core))):
            for chip in range(chips):
                at = pl.ds(pl.multiple_of((2 * chip + parity) * block, block), block)
                loads.append(pltpu.make_async_copy(source.at[chip, kind], to.at[:, at], weight_sems.at[kind, side, chip]))
        return loads
    weights = [weight_loads(kind, to) for kind, to in enumerate((wo, wg, wu, wd))]
    for load in [loads[0]] + weights[0] + loads[1:] + weights[1] + weights[2] + weights[3]: load.start()
    gsum_ref[...] = jnp.zeros_like(gsum_ref)
    enter()
    for load in [loads[0]] + weights[0]: load.wait()
    def project(index, carry):
        k, flow = index // 2, index % 2
        at = pl.ds(pl.multiple_of(flow * half + k * big, big), big)
        part1[at, :] = dot(y[at, :], wo[...], ((1,), (0,))).astype(bfloat)
        @pl.when(one.near(flow) == 0)
        def _():
            one.reduce(flow, 2 * k)
            one.reduce(flow, 2 * k + 1)
        return carry
    lax.fori_loop(0, count, project, 0)
    for load in loads[1:] + weights[1] + weights[2] + weights[3]: load.wait()
    outs = ((n2s, n2_hbm), (ms, m_hbm), (das, da_hbm), (dbs, db_hbm), (pds, pd_hbm))
    def out_copy(i, flow, at):
        return pltpu.make_async_copy(outs[i][0].at[flow], outs[i][1].at[at], out_sems.at[i, flow])
    def dh_copy(flow, at):
        return pltpu.make_async_copy(dhs.at[flow], dh_hbm.at[at], out_sems.at[5, flow])
    def dy_copy(flow, at):
        return pltpu.make_async_copy(dys.at[flow], dy_hbm.at[at], out_sems.at[6, flow])

    def normed(at):
        mixed = x[at, :].astype(single) + land1[at, :].astype(single)
        rho = lax.rsqrt(jnp.mean(mixed * mixed, axis=-1, keepdims=True) + 1e-06)
        return rho, mixed * rho

    def inner(flow, k):
        at = pl.ds(pl.multiple_of(flow * half + k * big, big), big)
        @pl.when(k > 0)
        def _():
            for i in range(5): out_copy(i, flow, at).wait()
        rho, standard = normed(at)
        n2 = (standard * gain_ref[...]).astype(bfloat)
        n2s[flow] = n2
        a = dot(n2, wg[...], ((1,), (1,)))
        b = dot(n2, wu[...], ((1,), (1,)))
        dm = dot(g[at, :], wd[...], ((1,), (1,)))
        phi = 0.5 * (1.0 + lax.erf(a * math.sqrt(0.5)))
        gelu = a * phi
        slope = phi + a * jnp.exp(-0.5 * a * a) * (1.0 / math.sqrt(2.0 * math.pi))
        m = (gelu * b).astype(bfloat)
        da = (dm * b * slope).astype(bfloat)
        db = (dm * gelu).astype(bfloat)
        ms[flow] = m
        das[flow] = da
        dbs[flow] = db
        p3 = dot(da, wg[...], ((1,), (0,))) + dot(db, wu[...], ((1,), (0,)))
        part3[at, :] = p3.astype(bfloat)
        gsum_ref[...] += jnp.sum(p3 * standard, axis=0, keepdims=True)
        pds[flow] = dot(m, wd[...], ((1,), (0,))).astype(bfloat)
        for i in range(5): out_copy(i, flow, at).start()

    def last(flow, k):
        at = pl.ds(pl.multiple_of(flow * half + k * big, big), big)
        @pl.when(k > 0)
        def _():
            dh_copy(flow, at).wait()
            dy_copy(flow, at).wait()
        rho, standard = normed(at)
        scaled = land3[at, :].astype(single) * gain_ref[...]
        dh = g[at, :].astype(single) + rho * (
            scaled - standard * jnp.mean(scaled * standard, axis=-1, keepdims=True))
        low = dh.astype(bfloat)
        dhs[flow] = low
        dys[flow] = dot(low, wo[...], ((1,), (1,)))
        dh_copy(flow, at).start()
        dy_copy(flow, at).start()

    lag = 1
    slots = count + 4 * (n - 1) + lag + 1
    def slot(index, carry):
        s, flow = index // 2, index % 2
        near = one.near(flow)
        r = s - near
        @pl.when((near > 0) & (r >= 0) & (r < count))
        def _(): one.reduce(flow, r)
        arrival = 2 * (n - 1) - near
        k = s - arrival
        @pl.when((k >= 0) & (k < count))
        def _():
            one.cast(flow, k)
            @pl.when(k % 2 == 1)
            def _(): inner(flow, k // 2)
        near3 = n - 1 - near
        q = s - arrival - lag
        @pl.when((q >= 0) & (q < count) & (q % 2 == 1))
        def _():
            two.reduce(flow, q - 1)
            two.reduce(flow, q)
        e = s - (3 * (n - 1) - lag * 0) - (n - 1 - near3) - lag
        @pl.when((e >= 0) & (e < count) & (e % 2 == 1))
        def _():
            two.cast(flow, e - 1)
            two.cast(flow, e)
            last(flow, e // 2)
        return carry
    lax.fori_loop(0, 2 * slots, slot, 0)
    total_copy = pltpu.make_async_copy(land1, total_hbm, in_sems.at[0])
    total_copy.start()
    one.finish()
    two.finish()
    for flow in (0, 1):
        at = pl.ds(flow * half, big)
        for i in range(5): out_copy(i, flow, at).wait()
        dh_copy(flow, at).wait()
        dy_copy(flow, at).wait()
    total_copy.wait()

def middle(y, x, g, own, other, gain, cid, rows=64):
    full, width = x.shape
    hidden = y.shape[1]
    half = full // 2
    count = half // rows
    big = 2 * rows
    any_ = pl.BlockSpec(memory_space=pl.ANY)
    vm = pl.BlockSpec(memory_space=pltpu.VMEM)
    S = jax.ShapeDtypeStruct
    V = pltpu.VMEM
    wide, slim = (full, width), (full, hidden)
    return pl.pallas_call(
        functools.partial(middle_kernel, rows),
        out_shape=[S(wide, bfloat), S(wide, bfloat), S(slim, bfloat), S(slim, bfloat), S(slim, bfloat),
                   S(wide, bfloat), S(wide, bfloat), S(slim, single), S((1, width), single)],
        in_specs=[any_] * 5 + [vm],
        out_specs=[any_] * 8 + [vm],
        scratch_shapes=[V(slim, bfloat), V(wide, bfloat), V(wide, bfloat)] + [V((hidden, width), bfloat)] * 4
            + [V(wide, bfloat)] * 4
            + [V((2, big, width), bfloat), V((2, big, hidden), bfloat), V((2, big, hidden), bfloat),
               V((2, big, hidden), bfloat), V((2, big, width), bfloat), V((2, big, width), bfloat), V((2, big, hidden), single)]
            + [pltpu.SemaphoreType.DMA((3,)), pltpu.SemaphoreType.DMA((4, 2, own.shape[0])), pltpu.SemaphoreType.DMA((7, 2))]
            + [pltpu.SemaphoreType.DMA((2, count))] * 8,
        compiler_params=pltpu.CompilerParams(collective_id=cid, has_side_effects=True, vmem_limit_bytes=VMEM_ALL),
        cost_estimate=pl.CostEstimate(flops=260 * 10**9, bytes_accessed=60 * 10**6, transcendentals=0),
    )(y, x, g, own, other, gain)


def others():
    me = lax.axis_index("seq")
    core = me + 1 - 2 * (me % 2)
    x = 2 - 4 * ((me // 2) % 2)
    y = 4 - 8 * (me // 4)
    return core, (me + x, me + y, me + x + y)


def greet(devices):
    barrier = pltpu.get_barrier_semaphore()
    for device in devices:
        pl.semaphore_signal(barrier, inc=1, device_id={"seq": device}, device_id_type=MESH)
    pl.semaphore_wait(barrier, len(devices))


def scatter_kernel(shape, *refs):
    lefts = len(shape)
    turned = [flag for flags in shape for flag in flags]
    k = len(turned)
    refs = list(refs)

    def take(count):
        return [refs.pop(0) for _ in range(count)]

    left_hbm, right_hbm, outs = take(lefts), take(k), take(k)
    left, right = take(lefts), take(k)
    flipped = {i: refs.pop(0) if turned[i] == 1 else right[i] for i in range(k) if turned[i]}
    near_stage, near_land, far_stage, far_land = take(k), take(k), take(k), take(k)
    load_sem, near_send, near_recv, far_send, far_recv = refs
    loads = [
        pltpu.make_async_copy(a, b, load_sem.at[i])
        for i, (a, b) in enumerate(zip(right_hbm + left_hbm, right + left))
    ]
    for load in loads:
        load.start()
    me = lax.axis_index("seq")
    core, chips = others()
    greet((core, *chips))
    rows = left[0].shape[1] // 8
    piece = 256
    for i in range(k):
        loads[i].wait()
        if turned[i] == 1:

            def flip(t, carry):
                at = pl.ds(pl.multiple_of(t * piece, piece), piece)
                flipped[i][:, at] = right[i][at, :].T
                return carry

            lax.fori_loop(0, right[i].shape[0] // piece, flip, 0)
    for load in loads[k:]:
        load.wait()

    def near_copy(i, r):
        return pltpu.make_async_remote_copy(
            src_ref=near_stage[i].at[r],
            dst_ref=near_land[i].at[r],
            send_sem=near_send.at[i, r],
            recv_sem=near_recv.at[i, r],
            device_id={"seq": core},
            device_id_type=MESH,
        )

    def far_copy(i, r, device):
        return pltpu.make_async_remote_copy(
            src_ref=far_stage[i].at[r - 1],
            dst_ref=far_land[i].at[r - 1],
            send_sem=far_send.at[i, r - 1],
            recv_sem=far_recv.at[i, r - 1],
            device_id={"seq": device},
            device_id_type=MESH,
        )

    def away(r):
        x = 2 - 4 * ((me // 2) % 2)
        y = 4 - 8 * (me // 4)
        return (r % 2) * x + (r // 2) * y

    def tiles(device, use):
        index = 0
        columns = pl.ds(pl.multiple_of(device * rows, rows), rows)
        for g, flags in enumerate(shape):
            block = left[g][:, columns]
            upright = None if all(flags) else block.T
            for flag in flags:
                if flag:
                    use(index, dot(flipped[index][...], block, ((1,), (0,))))
                else:
                    use(index, dot(upright, right[index][...], ((1,), (0,))))
                index += 1

    def step(t, carry):
        @pl.when(t < 4)
        def _():
            r = 3 - t

            def use(i, tile):
                near_stage[i][r] = tile.astype(bfloat)
                near_copy(i, r).start()

            tiles(core + away(r), use)

        @pl.when(t > 0)
        def _():
            r = 4 - t

            def use(i, tile):
                near_copy(i, r).wait_recv()
                pair = tile + near_land[i][r].astype(single)

                @pl.when(r > 0)
                def _():
                    far_stage[i][r - 1] = pair.astype(bfloat)
                    far_copy(i, r, me + away(r)).start()

                @pl.when(r == 0)
                def _():
                    outs[i][...] = pair

            tiles(me + away(r), use)

        return carry

    lax.fori_loop(0, 5, step, 0)
    for i in range(k):
        for r in (3, 2, 1):
            far_copy(i, r, me + away(r)).wait_recv()
        outs[i][...] += (far_land[i][0].astype(single) + far_land[i][1].astype(single)) + far_land[i][2].astype(single)
    for i in range(k):
        for r in range(4):
            near_copy(i, r).wait_send()
        for r in (1, 2, 3):
            far_copy(i, r, me + away(r)).wait_send()


def grads_scattered(groups, cid):
    shape = tuple(tuple(flag for _, flag in rights) for _, rights in groups)
    lefts = [left for left, _ in groups]
    rights = [right for _, rights in groups for right, _ in rights]
    turned = [flag for flags in shape for flag in flags]
    rows = lefts[0].shape[1] // lax.axis_size("seq")
    V = pltpu.VMEM
    any_ = pl.BlockSpec(memory_space=pl.ANY)
    vm = pl.BlockSpec(memory_space=pltpu.VMEM)
    k = len(rights)
    sizes = [
        ((right.shape[1], rows), (right.shape[0], rows))[flag - 1] if flag else (rows, right.shape[1])
        for right, flag in zip(rights, turned)
    ]

    def tile(count):
        return [V((count, *size), bfloat) for size in sizes]

    return pl.pallas_call(
        functools.partial(scatter_kernel, shape),
        out_shape=[jax.ShapeDtypeStruct(size, single) for size in sizes],
        in_specs=[any_] * (len(lefts) + k),
        out_specs=[vm] * k,
        scratch_shapes=[V(a.shape, bfloat) for a in lefts + rights]
        + [V(right.shape[::-1], bfloat) for right, flag in zip(rights, turned) if flag == 1]
        + tile(4)
        + tile(4)
        + tile(3)
        + tile(3)
        + [pltpu.SemaphoreType.DMA((len(lefts) + k,))]
        + [pltpu.SemaphoreType.DMA((k, 4))] * 2
        + [pltpu.SemaphoreType.DMA((k, 3))] * 2,
        compiler_params=pltpu.CompilerParams(
            collective_id=cid, has_side_effects=True, vmem_limit_bytes=VMEM_ALL
        ),
        cost_estimate=pl.CostEstimate(
            flops=80 * 10**9, bytes_accessed=30 * 10**6, transcendentals=0
        ),
    )(*lefts, *rights)


def products_scattered(groups, cid):
    count = lax.axis_size("seq")
    if count == 8:
        return grads_scattered(groups, cid)
    sums = []
    for left, rights in groups:
        for right, flag in rights:
            local = mm(right, left, ((flag - 1,), (0,))) if flag else mm(left, right, ((0,), (0,)))
            sums.append(
                lax.psum_scatter(
                    local.astype(bfloat), "seq", scatter_dimension=1 if flag else 0, tiled=True
                ).astype(single)
            )
    return sums


def orthogonal_kernel(x_ref, out_ref, current):
    parts, height, _ = x_ref.shape
    squares = jnp.zeros((height, 1), single)
    for i in range(parts):
        value = x_ref[i].astype(single)
        squares += jnp.sum(value * value, axis=1, keepdims=True)
    norm = jnp.sqrt(jnp.sum(squares, axis=0, keepdims=True)) + 1e-07
    for i in range(parts):
        value = x_ref[i].astype(single) / norm
        current[i] = value
        out_ref[i] = value.astype(bfloat)

    def newton(step, carry):
        gram = jnp.zeros((height, height), single)
        for i in range(parts):
            gram += dot(out_ref[i], out_ref[i], ((1,), (1,)))
        low = gram.astype(bfloat)
        poly = (coef_second * gram + coef_third * dot(low, low, ((1,), (0,)))).astype(bfloat)
        for i in range(parts):
            value = coef_first * current[i] + dot(poly, out_ref[i], ((1,), (0,)))
            current[i] = value
            out_ref[i] = value.astype(bfloat)
        return carry

    lax.fori_loop(0, 5, newton, 0)


def orthogonal(block):
    vm = pl.BlockSpec(memory_space=pltpu.VMEM)
    return pl.pallas_call(
        orthogonal_kernel,
        out_shape=jax.ShapeDtypeStruct(block.shape, bfloat),
        in_specs=[vm],
        out_specs=vm,
        scratch_shapes=[pltpu.VMEM(block.shape, single)],
        compiler_params=pltpu.CompilerParams(vmem_limit_bytes=48 << 20),
        cost_estimate=pl.CostEstimate(
            flops=20 * 10**9, bytes_accessed=4 * 10**6, transcendentals=0
        ),
    )(block)


def rotated(values, cosine, sine):
    width = values.shape[1]
    even = lax.broadcasted_iota(jnp.int32, values.shape, 1) % 2 == 0
    swapped = jnp.where(even, -pltpu.roll(values, width - 1, 1), pltpu.roll(values, 1, 1))
    return values * cosine + swapped * sine

def front_kernel(x_hbm, gain_ref, cos_ref, sin_ref, q_hbm, k_hbm, v_hbm, s_hbm,
                 q_full, k_full, v_full, s_full, gains, n1, qh, kh, vh, sh,
                 x, rho, wq, wk, wv, ws, fq, fk, fv, fs, aq, ak, av, as_, load_sem, store_sem, send_sem, recv_sem):
    masters = (q_hbm, v_hbm, k_hbm, s_hbm)
    singles = (fq, fv, fk, fs)
    lands = (wq, wv, wk, ws, gains)
    fulls = (q_full, v_full, k_full, s_full)
    turned = (False, True, False, True)
    accs = (aq, av, ak, as_)
    loads = [pltpu.make_async_copy(a, b, load_sem.at[i]) for i, (a, b) in enumerate(zip(masters + (x_hbm,), singles + (x,)))]
    for load in loads: load.start()
    me = lax.axis_index("seq")
    core, (by_x, by_y, by_both) = others()
    step = {1: 1 - 2 * (me % 2), 2: 2 - 4 * ((me // 2) % 2), 4: 4 - 8 * (me // 4)}
    def place(rel):
        return me + sum(step[bit] for bit in (1, 2, 4) if rel & bit)
    greet((core, by_x, by_y))
    sent = []
    def send(rel, i, to):
        there = lands[i].at[place(rel)]
        copy = pltpu.make_async_remote_copy(
            src_ref=there, dst_ref=there, send_sem=send_sem.at[rel ^ to, i, to // 2], recv_sem=recv_sem.at[rel ^ to, i],
            device_id={"seq": place(to)}, device_id_type=MESH)
        copy.start()
        sent.append(copy)
    def arrive(rel, i):
        here = lands[i].at[place(rel)]
        pltpu.make_async_remote_copy(
            src_ref=here, dst_ref=here, send_sem=send_sem.at[rel, i, 0], recv_sem=recv_sem.at[rel, i],
            device_id={"seq": core}, device_id_type=MESH).wait_recv()
    gains[me] = gain_ref[...].astype(bfloat).astype(single)
    for to in (2, 4, 1): send(0, 4, to)
    for i in range(4):
        loads[i].wait()
        lands[i][me] = singles[i][...].astype(bfloat)
        for to in (2, 4, 1): send(0, i, to)
    loads[4].wait()
    tokens = x.shape[0]
    piece = 256
    def scale(t, carry):
        at = pl.ds(pl.multiple_of(t * piece, piece), piece)
        value = x[at, :].astype(single)
        rho[at, :] = lax.rsqrt(jnp.mean(value * value, axis=-1, keepdims=True) + 1e-06)
        return carry
    lax.fori_loop(0, tokens // piece, scale, 0)
    rows = gain_ref.shape[1]
    def product(rel, first):
        low = place(rel) - me % 2
        columns = pl.ds(pl.multiple_of(low * rows, 2 * rows), 2 * rows)
        scales = jnp.concatenate([gains[low][0:1, :], gains[low + 1][0:1, :]], axis=1)
        def part(t, carry):
            at = pl.ds(pl.multiple_of(t * piece, piece), piece)
            normed = (x[at, columns].astype(single) * rho[at, :] * scales).astype(bfloat)
            n1[at, columns] = normed
            for i in range(4):
                if turned[i]:
                    value = dot(normed[:, :rows], lands[i][low], ((1,), (1,)))
                    value += dot(normed[:, rows:], lands[i][low + 1], ((1,), (1,)))
                else:
                    both = lands[i][pl.ds(low, 2)].reshape(2 * rows, lands[i].shape[2])
                    value = dot(normed, both, ((1,), (0,)))
                if first: accs[i][at, :] = value
                else: accs[i][at, :] += value
            return carry
        lax.fori_loop(0, tokens // piece, part, 0)
    for i in (4, 0, 1, 2, 3): arrive(1, i)
    product(0, True)
    def relay(rel, i):
        arrive(rel, i)
        send(rel, i, 1)
        if rel == 2 and i in (0, 1, 4): send(rel, i, 4)
        if rel == 4 and i in (2, 3): send(rel, i, 2)
    for i in (4, 0, 1, 2, 3):
        relay(2, i)
        relay(4, i)
    for i in (4, 0, 1, 2, 3): arrive(3, i)
    product(2, False)
    for i in (4, 0, 1, 2, 3): arrive(5, i)
    product(4, False)
    for i in (4, 0, 2, 1, 3):
        arrive(6, i)
        send(6, i, 1)
    for i in (4, 0, 2, 1, 3): arrive(7, i)
    count = lands[0].shape[0]
    stores = []
    for i in range(4):
        if turned[i]:
            for b in range(count):
                part = fulls[i].at[:, pl.ds(b * rows, rows)]
                stores.append(pltpu.make_async_copy(lands[i].at[b], part, store_sem.at[i, b]))
        else:
            stores.append(pltpu.make_async_copy(lands[i], fulls[i], store_sem.at[i, 0]))
    for store in stores: store.start()
    product(6, False)
    heads = qh.shape[0] // 2
    block = tokens // 2
    def finish(s, carry):
        at = pl.ds(pl.multiple_of(s * block, block), block)
        for h in range(heads):
            keys = slice(h * KEY, (h + 1) * KEY)
            qh[s * heads + h] = rotated(aq[at, keys], cos_ref[...], sin_ref[...]).astype(bfloat)
            kh[s * heads + h] = (rotated(ak[at, keys], cos_ref[...], sin_ref[...]) * KEY ** -0.5).astype(bfloat)
            vh[s * heads + h] = av[at, :][:, h * VAL : (h + 1) * VAL].astype(bfloat)
            sh[s * heads + h] = as_[at, :][:, h * VAL : (h + 1) * VAL]
        return carry
    lax.fori_loop(0, 2, finish, 0)
    for copy in sent: copy.wait_send()
    for store in stores: store.wait()

def front(x, gains, cosine, sine, wq, wk, wv, ws, cid):
    tokens, width = x.shape
    count = lax.axis_size("seq")
    rows = width // count
    block = tokens // 2
    heads = wq.shape[1] // KEY
    any_ = pl.BlockSpec(memory_space=pl.ANY)
    vm = pl.BlockSpec(memory_space=pltpu.VMEM)
    S, V = jax.ShapeDtypeStruct, pltpu.VMEM
    gathered = [(count, *w.shape) for w in (wq, wk, wv, ws)]
    return pl.pallas_call(
        front_kernel,
        out_shape=[S(g, bfloat) for g in gathered[:2]] + [S((w.shape[0], width), bfloat) for w in (wv, ws)] + [S((count, 8, rows), single), S(x.shape, bfloat),
            S((2 * heads, block, KEY), bfloat), S((2 * heads, block, KEY), bfloat), S((2 * heads, block, VAL), bfloat), S((2 * heads, block, VAL), single)],
        in_specs=[any_, vm, vm, vm] + [any_] * 4,
        out_specs=[any_] * 4 + [vm] * 6,
        scratch_shapes=[V(x.shape, bfloat), V((tokens, 1), single)] + [V(g, bfloat) for g in gathered]
            + [V(w.shape, single) for w in (wq, wk, wv, ws)] + [V((tokens, columns), single) for columns in (wq.shape[1], wk.shape[1], wv.shape[0], ws.shape[0])]
            + [pltpu.SemaphoreType.DMA((5,)), pltpu.SemaphoreType.DMA((4, count)), pltpu.SemaphoreType.DMA((8, 5, 3)), pltpu.SemaphoreType.DMA((8, 5))],
        compiler_params=pltpu.CompilerParams(collective_id=cid, has_side_effects=True, vmem_limit_bytes=VMEM_ALL),
        cost_estimate=pl.CostEstimate(flops=70 * 10**9, bytes_accessed=40 * 10**6, transcendentals=0),
    )(x, gains, cosine, sine, wq, wk, wv, ws)


def peers():
    me = lax.axis_index("seq")
    core, (by_x, by_y, by_both) = others()
    turn = core - me
    return core, by_x, by_y, by_x + turn, by_y + turn, by_both, by_both + turn

def decays(rate, length):
    t = lax.broadcasted_iota(jnp.int32, (length, 1), 0).astype(single)
    u = lax.broadcasted_iota(jnp.int32, (1, length), 1).astype(single)
    offsets = t - u
    mask = jnp.where(offsets >= 0, jnp.exp(-rate * jnp.maximum(offsets, 0.0)), 0.0)
    return mask, jnp.exp(-rate * (t + 1.0)), jnp.exp(-rate * (length - 1.0 - t)), jnp.exp(-rate * length)

class Exchange:
    def __init__(self, stage, land, stage_two, land_two, sems):
        self.stage, self.land, self.stage_two, self.land_two = stage, land, stage_two, land_two
        self.sends, self.recvs, self.sends_two, self.recvs_two = sems
        self.me = lax.axis_index("seq")
        self.peers = peers()
    def copy(self, two, i):
        stage, land = (self.stage_two, self.land_two) if two else (self.stage, self.land)
        sends, recvs = (self.sends_two, self.recvs_two) if two else (self.sends, self.recvs)
        return pltpu.make_async_remote_copy(
            src_ref=stage.at[self.peers[i]], dst_ref=land.at[self.me], send_sem=sends.at[i],
            recv_sem=recvs.at[i], device_id={"seq": self.peers[i]}, device_id_type=MESH)
    def arrived(self, two, i):
        land = self.land_two if two else self.land
        recvs = self.recvs_two if two else self.recvs
        sends = self.sends_two if two else self.sends
        here = land.at[self.peers[i]]
        pltpu.make_async_remote_copy(
            src_ref=here, dst_ref=here, send_sem=sends.at[i], recv_sem=recvs.at[i],
            device_id={"seq": self.peers[i]}, device_id_type=MESH).wait_recv()
    def start(self):
        for i in reversed(range(7)): self.copy(False, i).start()
        self.land[self.me] = self.stage[self.me]
    def turn(self, decay, reverse):
        for i in range(7): self.arrived(False, i)
        count = self.stage.shape[0]
        def step(index, running):
            position = count - 1 - index if reverse else index
            self.stage_two[position] = running.astype(bfloat)
            return decay * running + self.land[position].astype(single)
        lax.fori_loop(0, count, step, jnp.zeros(self.stage.shape[1:], single))
        for i in reversed(range(7)): self.copy(True, i).start()
        self.land_two[self.me] = self.stage_two[self.me]
    def end(self):
        for i in range(7): self.arrived(True, i)
    def state(self, b):
        count, _, part, width = self.land_two.shape
        return self.land_two[:, b].reshape(count * part, width)
    def finish(self):
        for i in range(7):
            self.copy(False, i).wait_send()
            self.copy(True, i).wait_send()

def retain_kernel(heads, q, k, v, s, rates, y, o, weights, state, stage, land, stage_two, land_two, *sems):
    blocks, length = q.shape[0], q.shape[1]
    count = stage.shape[0]
    exchange = Exchange(stage, land, stage_two, land_two, sems)
    greet(exchange.peers)
    rate = lambda h: rates[pl.ds(h, 1), 0:1]
    def local(b, carry):
        _, _, kd, _ = decays(rate(b % heads), length)
        low = (k[b].astype(single) * kd).astype(bfloat)
        piece = dot(low, v[b], ((0,), (0,))).astype(bfloat)
        stage[:, pl.ds(b, 1)] = piece.reshape(count, 1, piece.shape[0] // count, piece.shape[1])
        return carry
    lax.fori_loop(0, blocks, local, 0)
    exchange.start()
    def inside(b, carry):
        mask, _, _, _ = decays(rate(b % heads), length)
        low = (dot(q[b], k[b], ((1,), (1,))) * mask).astype(bfloat)
        weights[b] = low
        o[b] = dot(low, v[b], ((1,), (0,)))
        return carry
    lax.fori_loop(0, blocks, inside, 0)
    exchange.turn(whole_decays(rates, heads, blocks, length), False)
    exchange.end()
    def outer(sequence, carry):
        parts = []
        for h in range(heads):
            b = sequence * heads + h
            _, qd, _, _ = decays(rate(h), length)
            incoming = exchange.state(b)
            state[b] = incoming
            total = o[b] + dot((q[b].astype(single) * qd).astype(bfloat), incoming, ((1,), (0,)))
            o[b] = total
            rho = lax.rsqrt(jnp.mean(total * total, axis=-1, keepdims=True) + 1e-05)
            gate = s[b]
            parts.append((gate * jax.nn.sigmoid(gate) * total * rho).astype(bfloat))
        at = pl.ds(pl.multiple_of(sequence * length, length), length)
        y[at, :] = jnp.concatenate(parts, axis=1)
        return carry
    lax.fori_loop(0, blocks // heads, outer, 0)
    exchange.finish()

def exchange_scratch(count, blocks, keys, vals):
    return [pltpu.VMEM((count, blocks, keys // count, vals), bfloat)] * 4 + [pltpu.SemaphoreType.DMA((7,))] * 4

def retain(q, k, v, s, rates, cid):
    blocks, length, keys = q.shape
    vals = v.shape[2]
    heads = rates.shape[0]
    count = lax.axis_size("seq")
    vm = pl.BlockSpec(memory_space=pltpu.VMEM)
    S = jax.ShapeDtypeStruct
    return pl.pallas_call(
        functools.partial(retain_kernel, heads),
        out_shape=[S((blocks // heads * length, heads * vals), bfloat), S((blocks, length, vals), single),
                   S((blocks, length, length), bfloat), S((blocks, keys, vals), bfloat)],
        in_specs=[vm] * 5, out_specs=[vm] * 4,
        scratch_shapes=exchange_scratch(count, blocks, keys, vals),
        compiler_params=pltpu.CompilerParams(collective_id=cid, has_side_effects=True, vmem_limit_bytes=48 << 20),
        cost_estimate=pl.CostEstimate(flops=40 * 10**9, bytes_accessed=20 * 10**6, transcendentals=0),
    )(q, k, v, s, jnp.broadcast_to(rates[:, None], (heads, 128)))

def whole_decays(rates, heads, blocks, length):
    head = lax.broadcasted_iota(jnp.int32, (blocks, 1, 1), 0) % heads
    whole = jnp.zeros((blocks, 1, 1), single)
    for h in range(heads):
        whole = jnp.where(head == h, jnp.exp(-rates[h : h + 1, 0:1] * length).reshape(1, 1, 1), whole)
    return whole


def unretain_kernel(
    heads, grad_ref, q, k, v, s, o, weights, state, rates, cosine, sine,
    dq, dk, dv, ds, do, value_part, key_part, stage, land, stage_two, land_two, *sems,
):
    blocks, length = q.shape[0], q.shape[1]
    count = stage.shape[0]
    exchange = Exchange(stage, land, stage_two, land_two, sems)
    greet(exchange.peers)

    def rate(h):
        return rates[pl.ds(h, 1), 0:1]

    def at(sequence):
        return pl.ds(pl.multiple_of(sequence * length, length), length)

    def gates(sequence, carry):
        grads = grad_ref[at(sequence), :]
        for h in range(heads):
            b = sequence * heads + h
            grad = grads[:, h * VAL : (h + 1) * VAL]
            total, gate = o[b], s[b]
            sigmoid = jax.nn.sigmoid(gate)
            rho = lax.rsqrt(jnp.mean(total * total, axis=-1, keepdims=True) + 1e-05)
            slope = sigmoid * (1.0 + gate * (1.0 - sigmoid))
            ds[h * VAL : (h + 1) * VAL, at(sequence)] = (grad * (total * rho) * slope).astype(bfloat).T
            inner = grad * (gate * sigmoid)
            mean = jnp.mean(inner * total, axis=-1, keepdims=True)
            low = (rho * (inner - total * (rho * rho * mean))).astype(bfloat)
            do[b] = low
            _, qd, _, _ = decays(rate(h), length)
            piece = dot((q[b].astype(single) * qd).astype(bfloat), low, ((0,), (0,))).astype(bfloat)
            stage[:, pl.ds(b, 1)] = piece.reshape(count, 1, piece.shape[0] // count, piece.shape[1])
        return carry

    lax.fori_loop(0, blocks // heads, gates, 0)
    exchange.start()

    def inside(sequence, carry):
        for h in range(heads):
            b = sequence * heads + h
            mask, qd, _, _ = decays(rate(h), length)
            score = (dot(do[b], v[b], ((1,), (1,))) * mask).astype(bfloat)
            value_part[b] = dot(weights[b], do[b], ((0,), (0,)))
            turned = dot(score, k[b], ((1,), (0,))) + dot(do[b], state[b], ((1,), (1,))) * qd
            dq[at(sequence), h * KEY : (h + 1) * KEY] = rotated(turned, cosine[...], -sine[...]).astype(bfloat)
            key_part[b] = dot(score, q[b], ((0,), (0,)))
        return carry

    lax.fori_loop(0, blocks // heads, inside, 0)
    exchange.turn(whole_decays(rates, heads, blocks, length), True)
    exchange.end()

    def outer(sequence, carry):
        for h in range(heads):
            b = sequence * heads + h
            _, _, kd, _ = decays(rate(h), length)
            outgoing = exchange.state(b)
            low = (k[b].astype(single) * kd).astype(bfloat)
            value = value_part[b] + dot(low, outgoing, ((1,), (0,)))
            dv[h * VAL : (h + 1) * VAL, at(sequence)] = value.astype(bfloat).T
            turned = key_part[b] + dot(v[b], outgoing, ((1,), (1,))) * kd
            turned = rotated(turned, cosine[...], -sine[...]) * KEY ** (-0.5)
            dk[at(sequence), h * KEY : (h + 1) * KEY] = turned.astype(bfloat)
        return carry

    lax.fori_loop(0, blocks // heads, outer, 0)
    exchange.finish()


def unretain(grad, q, k, v, s, o, weights, state, rates, cosine, sine, cid):
    blocks, length, keys = q.shape
    vals = v.shape[2]
    heads = rates.shape[0]
    count = lax.axis_size("seq")
    rows = blocks // heads * length
    vm = pl.BlockSpec(memory_space=pltpu.VMEM)
    S, V = jax.ShapeDtypeStruct, pltpu.VMEM
    return pl.pallas_call(
        functools.partial(unretain_kernel, heads),
        out_shape=[S((rows, heads * keys), bfloat)] * 2 + [S((heads * vals, rows), bfloat)] * 2,
        in_specs=[vm] * 11,
        out_specs=[vm] * 4,
        scratch_shapes=[V(v.shape, bfloat), V(v.shape, single), V(q.shape, single)]
        + exchange_scratch(count, blocks, keys, vals),
        compiler_params=pltpu.CompilerParams(
            collective_id=cid, has_side_effects=True, vmem_limit_bytes=VMEM_ALL
        ),
        cost_estimate=pl.CostEstimate(
            flops=50 * 10**9, bytes_accessed=30 * 10**6, transcendentals=0
        ),
    )(grad, q, k, v, s, o, weights, state, jnp.broadcast_to(rates[:, None], (heads, 128)), cosine, sine)


def by_block(array, heads):
    rows, columns = array.shape
    parts = array.reshape(SEQS, rows // SEQS, heads, columns // heads).transpose(0, 2, 1, 3)
    return parts.reshape(SEQS * heads, rows // SEQS, columns // heads)


def by_row(array):
    blocks, length, columns = array.shape
    heads = blocks // SEQS
    parts = array.reshape(SEQS, heads, length, columns).transpose(0, 2, 1, 3)
    return parts.reshape(SEQS * length, heads * columns)


def rotate(values, cosine, sine):
    column = lax.broadcasted_iota(jnp.int32, values.shape, values.ndim - 1)
    swapped = jnp.where(
        column % 2 == 0, -jnp.roll(values, -1, axis=-1), jnp.roll(values, 1, axis=-1)
    )
    return values * cosine + swapped * sine


def projected(x, retention_gain, channel_gain, cosine, sine, weights):
    width = x.shape[1]
    heads = HEADS // lax.axis_size("head")
    gains = jnp.stack([retention_gain, channel_gain])
    if lax.axis_size("seq") == 8:
        gains = jnp.pad(gains, ((0, 6), (0, 0)))
        *fulls, gains, normed, q, k, v, s = front(x, gains, cosine, sine, *weights, 3)
        fulls = [full.reshape(width, -1) for full in fulls[:2]] + fulls[2:]
        return fulls, (gains[:, 0].reshape(-1), gains[:, 1].reshape(-1)), normed, (q, k, v, s)
    gains = lax.all_gather(gains.astype(bfloat), "seq", axis=1, tiled=True).astype(single)
    fulls = [
        lax.all_gather(weight.astype(bfloat), "seq", axis=i // 2, tiled=True)
        for i, weight in enumerate(weights)
    ]
    stream = x.astype(single)
    rho = lax.rsqrt(jnp.mean(stream * stream, axis=-1, keepdims=True) + 1e-06)
    normed = (stream * rho * gains[0]).astype(bfloat)
    q, k = [by_block(nn(normed, full), heads) for full in fulls[:2]]
    v, s = [by_block(nt(normed, full), heads) for full in fulls[2:]]
    q = rotate(q, cosine, sine).astype(bfloat)
    k = (rotate(k, cosine, sine) * KEY ** (-0.5)).astype(bfloat)
    return fulls, (gains[0], gains[1]), normed, (q, k, v.astype(bfloat), s)


def factors(rates, length):
    steps = jnp.arange(length, dtype=single)
    offsets = steps[:, None] - steps[None, :]
    every = jnp.tile(rates, SEQS)[:, None, None]
    mask = jnp.where(offsets >= 0, jnp.exp(-every * jnp.maximum(offsets, 0.0)), 0.0)
    steps = steps[None, :, None]
    return mask, jnp.exp(-every * (steps + 1.0)), jnp.exp(-every * (length - 1.0 - steps)), jnp.exp(-every * length)


def batched(spec, left, right):
    return jnp.einsum(spec, left, right, preferred_element_type=single)


def retained(q, k, v, s, rates):
    if lax.axis_size("seq") == 8:
        return retain(q, k, v, s, rates, 4)
    mask, qd, kd, whole = factors(rates, q.shape[1])
    local = batched("buk,buv->bkv", (k.astype(single) * kd).astype(bfloat), v)
    incoming = state_exchange(local, whole, False)
    weights = (batched("btk,buk->btu", q, k) * mask).astype(bfloat)
    o = batched("btu,buv->btv", weights, v)
    o = o + batched("btk,bkv->btv", (q.astype(single) * qd).astype(bfloat), incoming)
    rho = lax.rsqrt(jnp.mean(o * o, axis=-1, keepdims=True) + 1e-05)
    gated = (s * jax.nn.sigmoid(s) * o * rho).astype(bfloat)
    return by_row(gated), o, weights, incoming


def unretained(gated_grad, q, k, v, s, o, weights, incoming, rates, cosine, sine):
    heads = rates.shape[0]
    if lax.axis_size("seq") == 8:
        return unretain(gated_grad, q, k, v, s, o, weights, incoming, rates, cosine, sine, 5)
    mask, qd, kd, whole = factors(rates, q.shape[1])
    grad = by_block(gated_grad, heads)
    rho = lax.rsqrt(jnp.mean(o * o, axis=-1, keepdims=True) + 1e-05)
    sigmoid = jax.nn.sigmoid(s)
    ds = (grad * (o * rho) * (sigmoid * (1.0 + s * (1.0 - sigmoid)))).astype(bfloat)
    inner = grad * (s * sigmoid)
    do = (
        rho * (inner - o * (rho * rho * jnp.mean(inner * o, axis=-1, keepdims=True)))
    ).astype(bfloat)
    local = batched("btk,btv->bkv", (q.astype(single) * qd).astype(bfloat), do)
    outgoing = state_exchange(local, whole, True)
    score = (batched("btv,buv->btu", do, v) * mask).astype(bfloat)
    dv = batched("btu,btv->buv", weights, do)
    dv = dv + batched("buk,bkv->buv", (k.astype(single) * kd).astype(bfloat), outgoing)
    dq = batched("btu,buk->btk", score, k) + batched("btv,bkv->btk", do, incoming) * qd
    dk = batched("btu,btk->buk", score, q) + batched("buv,bkv->buk", v, outgoing) * kd
    dq = rotate(dq, cosine, -sine).astype(bfloat)
    dk = (rotate(dk, cosine, -sine) * KEY ** (-0.5)).astype(bfloat)
    return by_row(dq), by_row(dk), by_row(dv.astype(bfloat)).T, by_row(ds).T


def muon_sent(gradients, moments, turned, shift):
    heads_here = HEADS // lax.axis_size("head")
    count = lax.axis_size("seq")
    moments_updated, pieces = [], []
    for gradient, moment, flag in zip(gradients, moments, turned):
        new = 0.95 * moment + gradient
        moments_updated.append(new)
        advance = (gradient + 0.95 * new).astype(bfloat)
        if not flag:
            advance = advance.T
        blocks = advance.reshape(heads_here, advance.shape[0] // heads_here, advance.shape[1])
        pieces.append(jnp.pad(blocks, ((0, 0), (0, VAL - blocks.shape[1]), (0, 0))))
    outgoing = jnp.concatenate(pieces, axis=0)
    block_count, _, row_count = outgoing.shape
    if count >= block_count:
        spacing = count // block_count
        place = shift % spacing
        outgoing = jnp.pad(outgoing[:, None], ((0, 0), (place, spacing - 1 - place), (0, 0), (0, 0)))
        outgoing = outgoing.reshape(count, 1, VAL, row_count)
    else:
        owned = block_count // count
        outgoing = outgoing.reshape(owned, count, VAL, row_count).transpose(1, 0, 2, 3)
    return moments_updated, lax.all_to_all(outgoing, "seq", split_axis=0, concat_axis=0, tiled=True)


def muon_orthogonal(received):
    count, items, _, row_count = received.shape
    if row_count == 256:
        results = [orthogonal(received[:, i]) for i in range(items)]
        return jnp.stack(results, axis=1)
    parts = D // 256
    whole = received.transpose(1, 2, 0, 3).reshape(items, VAL, parts, 256).transpose(0, 2, 1, 3)
    whole = jnp.stack([orthogonal(whole[i]) for i in range(items)])
    whole = whole.transpose(0, 2, 1, 3).reshape(items, VAL, count, row_count)
    return whole.transpose(2, 0, 1, 3)


def muon_applied(results, masters, turned, shift):
    heads_here = HEADS // lax.axis_size("head")
    count = lax.axis_size("seq")
    block_count = len(masters) * heads_here
    returned = lax.all_to_all(results, "seq", split_axis=0, concat_axis=0, tiled=True)
    row_count = returned.shape[3]
    if count >= block_count:
        spacing = count // block_count
        updates = returned.reshape(block_count, spacing, VAL, row_count)[:, shift % spacing]
    else:
        updates = returned.transpose(1, 0, 2, 3).reshape(block_count, VAL, row_count)
    updated = []
    for position, (master, flag) in enumerate(zip(masters, turned)):
        width = master.shape[0 if flag else 1] // heads_here
        piece = updates[position * heads_here : (position + 1) * heads_here, :width]
        change = piece.reshape(heads_here * width, row_count)
        if not flag:
            change = change.T
        updated.append(master - change.astype(single) * (muon_rate * muon_scale * math.sqrt(D)))
    return updated


def shards(
    tokens,
    cotangent,
    decay_rates,
    retention_gain,
    channel_gain,
    query_weight,
    key_weight,
    value_weight,
    swish_weight,
    output_weight,
    gate_weight,
    up_weight,
    down_weight,
    query_moment,
    key_moment,
    value_moment,
    swish_moment,
    output_moment,
    gate_moment,
    up_moment,
    down_moment,
    retention_first,
    retention_second,
    channel_first,
    channel_second,
):
    heads_here = HEADS // lax.axis_size("head")
    seq_count, block_length, width = tokens.shape
    rows = seq_count * block_length
    value_weight, swish_weight = value_weight.T, swish_weight.T
    gate_weight, up_weight = gate_weight.T, up_weight.T
    value_moment, swish_moment = value_moment.T, swish_moment.T
    gate_moment, up_moment = gate_moment.T, up_moment.T
    four = jnp.stack([output_weight, gate_weight, up_weight, down_weight]).astype(bfloat)
    by_chip = four.shape[2] == 256
    if by_chip:
        own_four = chips_gathered(four)
    else:
        own_four, other_four = halves_gathered(four)
    x = tokens.reshape(rows, width)
    upstream_low = cotangent.reshape(rows, width)
    positions = (lax.axis_index("seq") * block_length + jnp.arange(block_length)).astype(single)
    pair_index = (jnp.arange(KEY) // 2).astype(single)
    frequency = jnp.exp(-log_base * pair_index / (KEY // 2 - 1))
    angles = positions[:, None] * frequency[None, :]
    cosine, sine = jnp.cos(angles), jnp.sin(angles)
    rates = lax.dynamic_slice(decay_rates, (lax.axis_index("head") * heads_here,), (heads_here,))
    (
        (query_full, key_full, value_full, swish_full),
        (retention_scale, channel_scale),
        normed_low,
        (query_blocks, key_blocks, value_blocks, swish_blocks),
    ) = projected(
        x,
        retention_gain,
        channel_gain,
        cosine,
        sine,
        [query_weight, key_weight, value_weight, swish_weight],
    )
    own_four, query_blocks = lax.optimization_barrier((own_four, query_blocks))
    if by_chip:
        other_four = sibling(own_four)
    gated_low, retained_blocks, weights_low, incoming_low = retained(
        query_blocks, key_blocks, value_blocks, swish_blocks, rates
    )
    (
        mixed_total,
        normed_two_low,
        activated_low,
        gate_low_grad,
        up_low_grad,
        down_partial,
        mixed_low,
        gated_grad,
        channel_local,
    ) = middle(gated_low, x, upstream_low, own_four, other_four, channel_scale[None, :], 1)
    query_low_grad, key_low_grad, value_turned_grad, swish_turned_grad = unretained(
        gated_grad,
        query_blocks,
        key_blocks,
        value_blocks,
        swish_blocks,
        retained_blocks,
        weights_low,
        incoming_low,
        rates,
        cosine,
        sine,
    )
    normed_one_partial = (
        nt(query_low_grad, query_full)
        + nt(key_low_grad, key_full)
        + tn(value_turned_grad, value_full)
        + tn(swish_turned_grad, swish_full)
    )
    stream = x.astype(single)
    rho_one = lax.rsqrt(jnp.mean(stream * stream, axis=-1, keepdims=True) + 1e-06)
    standard_one = stream * rho_one
    stream = x.astype(single)
    rho_one = lax.rsqrt(jnp.mean(stream * stream, axis=-1, keepdims=True) + 1e-06)
    standard_one = stream * rho_one
    gain_local = jnp.stack(
        [jnp.sum(normed_one_partial * standard_one, axis=0), channel_local[0]], axis=1
    )
    down_total = lax.psum(down_partial, "head")
    normed_low, partial_low, gain_local = lax.optimization_barrier(
        (normed_low, normed_one_partial.astype(bfloat), gain_local)
    )
    gain_pieces = gain_exchanged(gain_local)
    late = products_scattered(
        [
            (
                normed_low,
                [
                    (query_low_grad, 0),
                    (key_low_grad, 0),
                    (value_turned_grad, 2),
                    (swish_turned_grad, 2),
                ],
            )
        ],
        2,
    )
    late_turned = (False, False, True, True)
    late_moments, late_received = muon_sent(
        late, [query_moment, key_moment, value_moment, swish_moment], late_turned, 1
    )
    normed_two_low, late_first, down_total, gain_pieces = lax.optimization_barrier(
        (normed_two_low, late[0], down_total, gain_pieces)
    )
    partial_low, down_total = lax.optimization_barrier((partial_low, down_total))
    normed_one_grad = lax.psum(partial_low, "head").astype(single)
    early = products_scattered(
        [
            (mixed_low, [(gated_low, 1)]),
            (normed_two_low, [(gate_low_grad, 1), (up_low_grad, 1)]),
            (upstream_low, [(activated_low, 1)]),
        ],
        6,
    )
    early_turned = (True, True, True, True)
    early_moments, early_received = muon_sent(
        early, [output_moment, gate_moment, up_moment, down_moment], early_turned, 0
    )
    late_received, early_first = lax.optimization_barrier((late_received, early[0]))
    late_results = muon_orthogonal(late_received)
    late_updated = muon_applied(
        late_results, [query_weight, key_weight, value_weight, swish_weight], late_turned, 1
    )
    early_received, late_results = lax.optimization_barrier((early_received, late_results))
    early_updated = muon_applied(
        muon_orthogonal(early_received),
        [output_weight, gate_weight, up_weight, down_weight],
        early_turned,
        0,
    )
    gain_sums = gain_summed(gain_pieces)
    retention_sum, channel_sum = gain_sums[:, 0], gain_sums[:, 1]
    scaled_one = normed_one_grad * retention_scale
    input_gradient = (
        mixed_low.astype(single)
        + rho_one
        * (scaled_one - standard_one * jnp.mean(scaled_one * standard_one, axis=-1, keepdims=True))
    ).astype(bfloat)
    retention_gain_updated, retention_first_updated, retention_second_updated = adam_gain(
        retention_gain, retention_sum, retention_first, retention_second
    )
    channel_gain_updated, channel_first_updated, channel_second_updated = adam_gain(
        channel_gain, channel_sum, channel_first, channel_second
    )

    def placed(late_four, early_four):
        query, key, value, swish = late_four
        output, gate, up, down = early_four
        return query, key, value.T, swish.T, output, gate.T, up.T, down

    whole = (seq_count, block_length, width)
    block_out = (stream + mixed_total.astype(single) + down_total.astype(single)).astype(bfloat)
    return (
        block_out.reshape(whole),
        input_gradient.reshape(whole),
        retention_sum,
        channel_sum,
        *placed(late, early),
        retention_gain_updated,
        channel_gain_updated,
        *placed(late_updated, early_updated),
        *placed(late_moments, early_moments),
        retention_first_updated,
        retention_second_updated,
        channel_first_updated,
        channel_second_updated,
    )


def solution(mesh):
    placed = (
        P(None, "seq", None),
        P(None, "seq", None),
        P(),
        P("seq"),
        P("seq"),
        P("seq", "head"),
        P("seq", "head"),
        P("seq", "head"),
        P("seq", "head"),
        P("head", "seq"),
        P("seq", "head"),
        P("seq", "head"),
        P("head", "seq"),
        P("seq", "head"),
        P("seq", "head"),
        P("seq", "head"),
        P("seq", "head"),
        P("head", "seq"),
        P("seq", "head"),
        P("seq", "head"),
        P("head", "seq"),
        P("seq"),
        P("seq"),
        P("seq"),
        P("seq"),
    )
    return jax.shard_map(
        shards,
        mesh=mesh,
        in_specs=placed,
        out_specs=(
            P(None, "seq", None),
            P(None, "seq", None),
            P("seq"),
            P("seq"),
            P("seq", "head"),
            P("seq", "head"),
            P("seq", "head"),
            P("seq", "head"),
            P("head", "seq"),
            P("seq", "head"),
            P("seq", "head"),
            P("head", "seq"),
            P("seq"),
            P("seq"),
            P("seq", "head"),
            P("seq", "head"),
            P("seq", "head"),
            P("seq", "head"),
            P("head", "seq"),
            P("seq", "head"),
            P("seq", "head"),
            P("head", "seq"),
            P("seq", "head"),
            P("seq", "head"),
            P("seq", "head"),
            P("seq", "head"),
            P("head", "seq"),
            P("seq", "head"),
            P("seq", "head"),
            P("head", "seq"),
            P("seq"),
            P("seq"),
            P("seq"),
            P("seq"),
        ),
        check_vma=False,
    )
```
